512 devices in a mesh: dp: 4 (over x), expert: 32 (over z, y_hi, core), mp: 4 (over y_lo).
Axes of the slice: x: 4, y: 8 (y_hi: 2, y_lo: 4; y = y_hi * 4 + y_lo), z: 8, core: 2. Of those that a mesh axis runs over, the one named last changes fastest.
Arguments:
- tokens: bfloat16 [16384, 2048], P(('dp', 'expert'), 'mp'), parts along dimension 0, may hold values from -6 to 6
- routes: int32 [16384, 2], P(('dp', 'expert')), parts along dimension 0, may hold values from 0 to 7, all different within a row; in each aligned block of 128 rows (0 to 127, 128 to 255, ...) at most 48 rows name the same one
- gate_num: int32 [16384], P(('dp', 'expert')), parts along dimension 0, may hold values from 1 to 63
- capacity: int32 [8], replicated, may hold values from 24 to 48
- w_up: bfloat16 [2048, 57344], P(None, ('expert', 'mp')), may hold values from -0.125 to 0.125
- w_down: bfloat16 [57344, 2048], P(('expert', 'mp')), may hold values from -0.0625 to 0.0625
Outputs:
- mixed: bfloat16 [16384, 2048], P(('dp', 'expert'), 'mp'), parts along dimension 0
The draws below stay inside these ranges and needn't reach their ends.
There are 4 independent parts, one for each index of `dp`. The reference program is written for one: setup_inputs(seed, part) draws one part's arguments, and reference() takes and returns one part's arrays. A program takes and returns all parts, laid end to end along the dimension named above; an argument that names none is the same for every part. Nothing has to cross between parts.
Inputs may be any that keep to these rules, and one draw needn't show every extreme that they name: `routes`: each row names two different experts; in each aligned block of 128 rows no expert is named by more than 48 rows, a bound that some block reaches.
All inputs are finite; a program needn't handle non-finite values.
Results may differ from the reference program's by a relative error of at most 0.0085.
Values may be sent and summed in bfloat16 or wider, within the bound.
No kernel may reach another device: no remote copies, remote signals or barrier semaphores. Data moves between devices by JAX's collectives and lax.ppermute only.
A program may use at most 64 MiB of HBM per device.

```python
import math
import jax
import jax.numpy as jnp
import numpy as np
from jax import lax

D = 2048
FF = 7168
TOK_DEV = 128
GROUP = 4
EXPERTS = 8
CAP = 48
TOKENS = 4096
N_EXPERT = 32
N_MP = 4


def with_ends(drawn, own_key, smallest, largest):
    index_at = [jax.random.randint(jax.random.fold_in(own_key, axis), (), 0, length) for axis, length in enumerate(drawn.shape)]
    widest = drawn.shape.index(max(drawn.shape))
    neighbour = index_at[:widest] + [(index_at[widest] + 1) % drawn.shape[widest]] + index_at[widest + 1:]
    return drawn.at[tuple(index_at)].set(smallest).at[tuple(neighbour)].set(largest)


def block_levels(rng, dims, cuts, low, top_value):
    loudness = 1.0
    for axis_at, shards_of in cuts:
        draws = jax.random.uniform(jax.random.fold_in(jax.random.fold_in(rng, 6), axis_at), (shards_of,), jnp.float32, low / len(cuts), top_value / len(cuts))
        loudness = loudness * jnp.repeat(jnp.exp(draws), dims[axis_at] // shards_of).reshape((-1,) + (1,) * (len(dims) - 1 - axis_at))
    return loudness


def shared_out(key, own, number, rows, count, top, limit, lean):
    order = jax.random.permutation(key, count)
    heavy_load, ordinary = portions_of(count, rows * top, limit, lean, True), portions_of(count, rows * top, limit, lean, False)
    places = jnp.arange(count)

    def named(sizes, offset_by):
        used = int((sizes > 0).sum())
        fixed = max(1, used // 4)
        shifted = fixed + (places - fixed + offset_by * (used - fixed)) % max(1, count - fixed)
        return jnp.zeros((count,), jnp.int32).at[order[jnp.where(places < fixed, places, shifted)]].set(jnp.asarray(sizes, jnp.int32))

    sizes = jnp.where(number % 4 == 0, named(heavy_load, number // 4), named(ordinary, number - number // 4 - 1))
    mixed = jax.random.permutation(jax.random.fold_in(own, 3), count)
    donor, taker = mixed[0:count // 2 * 2:2], mixed[1:count // 2 * 2:2]
    margin = jnp.minimum(sizes[donor] - 1, limit - sizes[taker]) // 2
    margin = jnp.where((donor == order[0]) | (taker == order[0]) | (sizes[taker] == 0), 0, jnp.maximum(margin, 0))
    shifted = jax.random.randint(jax.random.fold_in(own, 4), (count // 2,), 0, 1 << 20) % (margin + 1)
    sizes = sizes.at[donor].add(-shifted).at[taker].add(shifted)
    labels = jnp.searchsorted(jnp.cumsum(sizes), jnp.arange(rows * top), side="right").astype(jnp.int32)
    listing = labels.reshape(top, rows).T
    listing = listing[jax.random.permutation(jax.random.fold_in(own, 1), rows)]
    offset_by = jax.random.randint(jax.random.fold_in(own, 2), (rows, 1), 0, top)
    return jnp.take_along_axis(listing, (jnp.arange(top)[None, :] + offset_by) % top, axis=1)


def portions_of(number_of, total, bound, lean, full):
    loads = [(1 << 20) // math.isqrt(rank ** lean) + 1 for rank in range(1, number_of + 1)]
    largest = bound if full else min(bound, max(-(-total // number_of), total * loads[0] // sum(loads)))
    least = 1 if total - largest >= number_of - 1 else 0
    given, surplus = [largest] + [least] * (number_of - 1), total - largest - least * (number_of - 1)
    while surplus > 0:
        candidates = [i for i in range(1, number_of) if given[i] < largest] or [i for i in range(1, number_of) if given[i] < bound]
        mass, remaining = sum([loads[i] for i in candidates]), surplus
        for i in candidates:
            addition = min(bound - given[i], max(1, remaining * loads[i] // mass), surplus)
            given[i] = given[i] + addition
            surplus = surplus - addition
    return np.array(given)


def normal_values(key, shape, scale, limit, shards=(), held_as=jnp.bfloat16):
    array = jax.random.normal(key, shape, jnp.float32) * scale
    if len(shards) > 0:
        array = block_levels(key, shape, shards, -0.22, 0.18) * array
    return jnp.clip(array, min=-limit, max=limit).astype(held_as)


def setup_inputs(seed: int = 0, part: int = 0) -> dict:
    arg_keys = jax.random.split(jax.random.key(seed), 7)
    part_keys = jax.random.split(jax.random.fold_in(arg_keys[6], part), 7)
    tokens = normal_values(part_keys[0], (TOKENS, D), 1.0, 6.0, ((0, 32), (1, 4)))
    routes_keys = jax.random.split(jax.random.fold_in(part_keys[1], 1), TOKENS // TOK_DEV)
    routes_turns = jax.random.permutation(jax.random.fold_in(part_keys[1], 3), TOKENS // TOK_DEV)
    routes = jax.vmap(lambda own, number: shared_out(jax.random.fold_in(part_keys[1], 2), own, number, TOK_DEV, EXPERTS, 2, CAP, 2))(routes_keys, routes_turns).reshape((TOKENS, 2))
    gate_num = with_ends(jax.random.randint(part_keys[2], (TOKENS,), 1, 64), jax.random.fold_in(part_keys[2], 1), 1, 63).astype(jnp.int32)
    capacity = with_ends(jax.random.randint(arg_keys[3], (EXPERTS,), CAP // 2, CAP + 1), jax.random.fold_in(arg_keys[3], 1), CAP // 2, CAP).astype(jnp.int32)
    w_up = normal_values(arg_keys[4], (D, EXPERTS * FF), D ** -0.5, 0.125, ((1, 128),))
    w_down = normal_values(arg_keys[5], (EXPERTS * FF, D), FF ** -0.5, 0.0625, ((0, 128),))
    return {"tokens": tokens, "routes": routes, "gate_num": gate_num, "capacity": capacity, "w_up": w_up, "w_down": w_down}


def reference(tokens, routes, gate_num, capacity, w_up, w_down):
    shard_count = GROUP * N_MP
    shard_width = FF // shard_count
    row_count = N_EXPERT * CAP
    expert_ids = jnp.arange(EXPERTS, dtype=jnp.int32)
    named_count = (routes[:, :, None] == expert_ids[None, None, :]).astype(jnp.int32).sum(axis=1)
    blocked = named_count.reshape(N_EXPERT, TOK_DEV, EXPERTS)
    positions = (jnp.cumsum(blocked, axis=1) - blocked).reshape(TOKENS, EXPERTS)
    route_pos = jnp.take_along_axis(positions, routes, axis=1)
    kept_mask = route_pos < capacity[routes]
    first_share = gate_num.astype(jnp.float32) / 64.0
    weights = jnp.stack([first_share, 1.0 - first_share], axis=1)
    source_block = jnp.arange(TOKENS, dtype=jnp.int32) // TOK_DEV
    slot_index = source_block[:, None] * CAP + route_pos
    token_ids = jnp.arange(2 * TOKENS, dtype=jnp.int32) // 2
    token_copies = tokens[token_ids]

    def per_expert(expert):
        chosen = (routes == expert) & kept_mask
        target = jnp.where(chosen, slot_index, row_count).reshape(-1).astype(jnp.int32)
        slot_rows = jnp.zeros((row_count + 1, D), jnp.bfloat16).at[target].set(token_copies)[:row_count]
        up_cols = lax.dynamic_slice_in_dim(w_up, expert * FF, FF, 1)
        hidden = jax.nn.silu(jnp.dot(slot_rows, up_cols, preferred_element_type=jnp.float32)).astype(jnp.bfloat16)
        down_rows = lax.dynamic_slice_in_dim(w_down, expert * FF, FF, 0)

        def add_shard(running, shard_id):
            hidden_part = lax.dynamic_slice_in_dim(hidden, shard_id * shard_width, shard_width, 1)
            down_part = lax.dynamic_slice_in_dim(down_rows, shard_id * shard_width, shard_width, 0)
            partial_value = jnp.dot(hidden_part, down_part, preferred_element_type=jnp.float32).astype(jnp.bfloat16)
            partial_value = lax.optimization_barrier(partial_value)
            return running + partial_value.astype(jnp.float32), None

        start = jnp.zeros((row_count, D), jnp.float32)
        return lax.scan(add_shard, start, jnp.arange(shard_count, dtype=jnp.int32))[0]

    expert_out = lax.map(per_expert, expert_ids)
    flat_index = (routes * row_count + jnp.where(kept_mask, slot_index, 0)).astype(jnp.int32)
    values = expert_out.reshape(EXPERTS * row_count, D)[flat_index]
    scaled = jnp.where(kept_mask, weights, 0.0)
    mixed = jnp.sum(scaled[:, :, None] * values, axis=1)
    return mixed.astype(jnp.bfloat16)
```

```python
import jax
import jax.numpy as jnp
from jax import lax
from jax.experimental import pallas as pl
from jax.experimental.pallas import tpu as pltpu
from jax.sharding import Mesh, PartitionSpec as P

EXPERTS = 8


def ffn_body(x_ref, up_ref, down_ref, out_ref):
    chunks, rows, width = x_ref.shape
    acc = jnp.zeros((rows, up_ref.shape[0]), jnp.float32)
    for m in range(chunks):
        acc += lax.dot_general(
            x_ref[m],
            up_ref[:, m * width : (m + 1) * width],
            (((1,), (1,)), ((), ())),
            preferred_element_type=jnp.float32,
        )
    hidden = (acc / (1.0 + jnp.exp(-acc))).astype(jnp.bfloat16)
    for m in range(chunks):
        out_ref[m] = jnp.dot(
            hidden,
            down_ref[:, m * width : (m + 1) * width],
            preferred_element_type=jnp.float32,
        ).astype(jnp.bfloat16)


def ffn(x, up_t, down):
    groups, chunks, rows, width = x.shape
    hidden, features = up_t.shape
    block = pl.BlockSpec((None, chunks, rows, width), lambda g: (g, 0, 0, 0))
    whole = pl.BlockSpec((hidden, features), lambda g: (0, 0))
    return pl.pallas_call(
        ffn_body,
        grid=(groups,),
        in_specs=[block, whole, whole],
        out_specs=block,
        out_shape=jax.ShapeDtypeStruct(x.shape, jnp.bfloat16),
        compiler_params=pltpu.CompilerParams(dimension_semantics=("arbitrary",)),
        name="ffn",
    )(x, up_t, down)


def routing(routes, gate_num, capacity, slot_count):
    token_count = routes.shape[0]
    expert_count = capacity.shape[0]
    expert_ids = jnp.arange(expert_count, dtype=jnp.int32)
    matches = routes[:, :, None] == expert_ids[None, None, :]
    named_count = matches.sum(axis=1).astype(jnp.bfloat16)
    token_ids = jnp.arange(token_count, dtype=jnp.int32)
    lower_mask = (token_ids[:, None] > token_ids[None, :]).astype(jnp.bfloat16)
    positions = jnp.dot(
        lower_mask, named_count, preferred_element_type=jnp.float32
    ).astype(jnp.int32)
    route_pos = jnp.sum(jnp.where(matches, positions[:, None, :], 0), axis=2)
    route_cap = jnp.sum(jnp.where(matches, capacity[None, None, :], 0), axis=2)
    kept_mask = route_pos < route_cap
    slot_index = jnp.where(kept_mask, routes * slot_count + route_pos, -1)
    first_share = gate_num.astype(jnp.float32) / 64.0
    weights = jnp.where(kept_mask, jnp.stack([first_share, 1.0 - first_share], axis=1), 0.0)
    slot_ids = jnp.arange(expert_count * slot_count, dtype=jnp.int32)
    dispatch = jnp.any(slot_ids[:, None, None] == slot_index[None, :, :], axis=2)
    combine_hits = slot_ids[None, :, None] == slot_index[:, None, :]
    combine = jnp.sum(jnp.where(combine_hits, weights[:, None, :], 0.0), axis=2)
    return dispatch.astype(jnp.bfloat16), combine


def per_device(tokens, routes, gate_num, capacity, w_up, w_down):
    expert_count = capacity.shape[0]
    token_count, width = tokens.shape
    slot_count = min(token_count, 3 * token_count // expert_count)
    plane = ("yh", "core", "mp")
    chunks = lax.axis_size("mp")
    dispatch, combine = routing(routes, gate_num, capacity, slot_count)
    rows = jnp.dot(dispatch, tokens, preferred_element_type=jnp.float32).astype(jnp.bfloat16)
    sent = lax.all_to_all(
        rows.reshape(expert_count, slot_count, width), "z", 0, 0, tiled=True
    ).reshape(expert_count * slot_count, width)
    whole = lax.all_gather(sent, plane)
    groups = whole.shape[0] // chunks
    x = whole.reshape(groups, chunks, expert_count * slot_count, width)
    partial_value = ffn(x, w_up.T, w_down)
    summed = lax.psum_scatter(
        partial_value.reshape(groups * chunks, expert_count * slot_count, width), plane
    )
    back = lax.all_to_all(
        summed.reshape(expert_count, slot_count, width), "z", 0, 0, tiled=True
    ).reshape(expert_count * slot_count, width)
    mixed = jnp.dot(
        combine,
        back.astype(jnp.float32),
        precision=lax.Precision.HIGHEST,
        preferred_element_type=jnp.float32,
    )
    return mixed.astype(jnp.bfloat16)


def solution(mesh):
    sizes = dict(mesh.shape)
    group = sizes["expert"] // EXPERTS
    devices = mesh.devices.reshape(sizes["dp"], EXPERTS, group // 2, 2, sizes["mp"])
    fine = Mesh(devices, ("dp", "z", "yh", "core", "mp"))
    expert = ("z", "yh", "core")
    return jax.shard_map(
        per_device,
        mesh=fine,
        in_specs=(
            P(("dp", *expert), "mp"),
            P(("dp", *expert), None),
            P(("dp", *expert)),
            P(),
            P(None, (*expert, "mp")),
            P((*expert, "mp"), None),
        ),
        out_specs=P(("dp", *expert), "mp"),
        check_vma=False,
    )
```

```python
import jax
import jax.numpy as jnp
from jax import lax
from jax.experimental import pallas as pl
from jax.experimental.pallas import tpu as pltpu
from jax.sharding import Mesh, PartitionSpec as P

EXPERTS = 8
RING = ("yh", "mp")
STREAMS = 2


def ffn_body(place_ref, *refs):
    count = (len(refs) - 6) // 2
    x_refs, (up_a, up_b, down_a, down_b) = refs[:count], refs[count : count + 4]
    out_refs, (x_all, out_all) = refs[count + 4 : -2], refs[-2:]
    rows, width = x_refs[0].shape
    chunks = x_all.shape[1] // width
    place = place_ref[0]

    def spot(j):
        source = lax.rem(place + j, count)
        row = pl.multiple_of(lax.div(source, chunks) * rows, rows)
        col = pl.multiple_of(lax.rem(source, chunks) * width, width)
        return pl.ds(row, rows), pl.ds(col, width)

    for j in range(count):
        x_all[spot(j)] = x_refs[j][...]
    hidden = []
    for up in (up_a, up_b):
        acc = lax.dot_general(
            x_all[...], up[...], (((1,), (1,)), ((), ())), preferred_element_type=jnp.float32
        )
        hidden.append((acc / (1.0 + jnp.exp(-acc))).astype(jnp.bfloat16))
    for m in range(chunks):
        cols = slice(m * width, (m + 1) * width)
        total = jnp.dot(hidden[0], down_a[:, cols], preferred_element_type=jnp.float32)
        total += jnp.dot(hidden[1], down_b[:, cols], preferred_element_type=jnp.float32)
        out_all[:, cols] = total.astype(jnp.bfloat16)
    for j in range(count):
        out_refs[j][...] = out_all[spot(j)]


def ffn(place, chunks, weights, features):
    rows, width = chunks[0].shape
    count = len(chunks)
    total_rows = rows * count * width // features
    vmem = pl.BlockSpec(memory_space=pltpu.VMEM)
    return pl.pallas_call(
        ffn_body,
        in_specs=[pl.BlockSpec(memory_space=pltpu.SMEM)] + [vmem] * (count + 4),
        out_specs=[vmem] * count,
        out_shape=[jax.ShapeDtypeStruct((rows, width), jnp.bfloat16)] * count,
        scratch_shapes=[pltpu.VMEM((total_rows, features), jnp.bfloat16)] * 2,
        compiler_params=pltpu.CompilerParams(vmem_limit_bytes=20 << 20),
        name="ffn",
    )(place, *chunks, *weights)


def routing(routes, gate_num, capacity, slot_count):
    token_count = routes.shape[0]
    expert_count = capacity.shape[0]
    expert_ids = jnp.arange(expert_count, dtype=jnp.int32)
    matches = routes[:, :, None] == expert_ids[None, None, :]
    named_count = matches.sum(axis=1).astype(jnp.bfloat16)
    token_ids = jnp.arange(token_count, dtype=jnp.int32)
    lower_mask = (token_ids[:, None] > token_ids[None, :]).astype(jnp.bfloat16)
    positions = jnp.dot(
        lower_mask, named_count, preferred_element_type=jnp.float32
    ).astype(jnp.int32)
    route_pos = jnp.sum(jnp.where(matches, positions[:, None, :], 0), axis=2)
    route_cap = jnp.sum(jnp.where(matches, capacity[None, None, :], 0), axis=2)
    kept_mask = route_pos < route_cap
    part = slot_count // STREAMS
    stream = route_pos // part
    slot_index = (stream * expert_count + routes) * part + route_pos - stream * part
    slot_index = jnp.where(kept_mask, slot_index, -1)
    first_share = gate_num.astype(jnp.float32) / 64.0
    weights = jnp.where(kept_mask, jnp.stack([first_share, 1.0 - first_share], axis=1), 0.0)
    slot_ids = jnp.arange(expert_count * slot_count, dtype=jnp.int32)
    dispatch = jnp.any(slot_ids[:, None, None] == slot_index[None, :, :], axis=2)
    combine_hits = slot_ids[None, :, None] == slot_index[:, None, :]
    combine = jnp.sum(jnp.where(combine_hits, weights[:, None, :], 0.0), axis=2)
    return dispatch.astype(jnp.bfloat16), combine.astype(jnp.bfloat16)


def shift(value, axis, by):
    count = lax.axis_size(axis)
    return lax.ppermute(value, axis, [(i, (i + by) % count) for i in range(count)])


def add(a, b):
    return (a.astype(jnp.float32) + b.astype(jnp.float32)).astype(jnp.bfloat16)


def per_device(tokens, routes, gate_num, capacity, w_up, w_down):
    expert_count = capacity.shape[0]
    token_count, width = tokens.shape
    features = w_up.shape[0]
    slot_count = min(token_count, 3 * token_count // expert_count)
    part = slot_count // STREAMS
    count = lax.axis_size(RING)
    half = count // 2
    place = lax.axis_index(RING).astype(jnp.int32).reshape(1)
    up = w_up.T
    weights = (up, shift(up, "core", 1), w_down, shift(w_down, "core", 1))
    dispatch, combine = routing(routes, gate_num, capacity, slot_count)
    rows = jnp.dot(dispatch, tokens, preferred_element_type=jnp.float32).astype(jnp.bfloat16)
    rows = rows.reshape(STREAMS, expert_count, part, width)

    held = []
    for s in range(STREAMS):
        mine = lax.all_to_all(rows[s], "z", 0, 0, tiled=True)
        held.append({0: mine.reshape(expert_count * part, width)})
    last = (-half, half)
    for step in range(1, half + 1):
        for s in range(STREAMS):
            if step < half or last[s] < 0:
                held[s][-step] = shift(held[s][1 - step], RING, 1)
            if step < half or last[s] > 0:
                held[s][step] = shift(held[s][step - 1], RING, -1)

    own = []
    for s in range(STREAMS):
        order = [j if j in held[s] else j - count for j in range(count)]
        own.append(ffn(place, [held[s][j] for j in order], weights, features))

    ahead, behind = [None] * STREAMS, [None] * STREAMS
    for step in range(half, 0, -1):
        for s in range(STREAMS):
            if step < half or last[s] < 0:
                sent = own[s][step]
                sent = sent if ahead[s] is None else add(sent, ahead[s])
                ahead[s] = shift(sent, RING, 1)
            if step < half or last[s] > 0:
                sent = own[s][count - step]
                sent = sent if behind[s] is None else add(sent, behind[s])
                behind[s] = shift(sent, RING, -1)

    back = []
    for s in range(STREAMS):
        total = own[s][0].astype(jnp.float32) + ahead[s].astype(jnp.float32)
        total = (total + behind[s].astype(jnp.float32)).astype(jnp.bfloat16)
        total = total.reshape(expert_count, part, width)
        back.append(lax.all_to_all(total, "z", 0, 0, tiled=True).reshape(-1, width))
    length = expert_count * part
    mixed = jnp.zeros((token_count, width), jnp.float32)
    for s in range(STREAMS):
        mixed += jnp.dot(
            combine[:, s * length : (s + 1) * length],
            back[s],
            preferred_element_type=jnp.float32,
        )
    return mixed.astype(jnp.bfloat16)


def solution(mesh):
    sizes = dict(mesh.shape)
    group = sizes["expert"] // EXPERTS
    devices = mesh.devices.reshape(sizes["dp"], EXPERTS, group // 2, 2, sizes["mp"])
    fine = Mesh(devices, ("dp", "z", "yh", "core", "mp"))
    expert = ("z", "yh", "core")
    return jax.shard_map(
        per_device,
        mesh=fine,
        in_specs=(
            P(("dp", *expert), "mp"),
            P(("dp", *expert), None),
            P(("dp", *expert)),
            P(),
            P(None, (*expert, "mp")),
            P((*expert, "mp"), None),
        ),
        out_specs=P(("dp", *expert), "mp"),
        check_vma=False,
    )
```

```python
import jax
import jax.numpy as jnp
from jax import lax
from jax.experimental import pallas as pl
from jax.experimental.pallas import tpu as pltpu
from jax.sharding import Mesh, PartitionSpec as P


EXPERTS = 8
CIRCLE = ("yh", "mp")
OFFSETS = (0, -1, -2, -3, -4, 1, 2, 3)


def ffn_body(place_ref, *refs):
    count = len(OFFSETS)
    x_refs, (up_a, up_b, down_a, down_b) = refs[:count], refs[count : count + 4]
    out_refs, (x_all, out_all) = refs[count + 4 : -2], refs[-2:]
    rows, width = x_refs[0].shape
    chunks = x_all.shape[1] // width

    def spot(offset):
        source = lax.rem(place_ref[0] + place_ref[1] * offset + count, count)
        row = pl.multiple_of(lax.div(source, chunks) * rows, rows)
        col = pl.multiple_of(lax.rem(source, chunks) * width, width)
        return pl.ds(row, rows), pl.ds(col, width)

    for x_ref, offset in zip(x_refs, OFFSETS):
        x_all[spot(offset)] = x_ref[...]
    hidden = []
    for up in (up_a, up_b):
        acc = lax.dot_general(
            x_all[...], up[...], (((1,), (1,)), ((), ())), preferred_element_type=jnp.float32
        )
        hidden.append((acc / (1.0 + jnp.exp(-acc))).astype(jnp.bfloat16))
    for m in range(chunks):
        cols = slice(m * width, (m + 1) * width)
        total = jnp.dot(hidden[0], down_a[:, cols], preferred_element_type=jnp.float32)
        total += jnp.dot(hidden[1], down_b[:, cols], preferred_element_type=jnp.float32)
        out_all[:, cols] = total.astype(jnp.bfloat16)
    for j, out_ref in enumerate(out_refs[:-1]):
        out_ref[...] = out_all[spot(j)]
    for j in range(out_refs[-1].shape[0]):
        out_refs[-1][j] = out_all[spot(-1 - j)]


def ffn(place, chunks, weights, features):
    rows, width = chunks[0].shape
    count = len(chunks)
    total_rows = rows * count * width // features
    vmem = pl.BlockSpec(memory_space=pltpu.VMEM)
    shapes = [(rows, width)] * (count // 2 + 1) + [(count // 2 - 1, rows, width)]
    return pl.pallas_call(
        ffn_body,
        in_specs=[pl.BlockSpec(memory_space=pltpu.SMEM)] + [vmem] * (count + 4),
        out_specs=[vmem] * len(shapes),
        out_shape=[jax.ShapeDtypeStruct(shape, jnp.bfloat16) for shape in shapes],
        scratch_shapes=[pltpu.VMEM((total_rows, features), jnp.bfloat16)] * 2,
        compiler_params=pltpu.CompilerParams(vmem_limit_bytes=16 << 20),
        name="ffn",
    )(place, *chunks, *weights)


def routing(routes, gate_num, capacity, slot_count):
    token_count = routes.shape[0]
    expert_count = capacity.shape[0]
    expert_ids = jnp.arange(expert_count, dtype=jnp.int32)
    matches = routes[:, :, None] == expert_ids[None, None, :]
    named_count = matches.sum(axis=1).astype(jnp.bfloat16)
    token_ids = jnp.arange(token_count, dtype=jnp.int32)
    lower_mask = (token_ids[:, None] > token_ids[None, :]).astype(jnp.bfloat16)
    positions = jnp.dot(
        lower_mask, named_count, preferred_element_type=jnp.float32
    ).astype(jnp.int32)
    route_pos = jnp.sum(jnp.where(matches, positions[:, None, :], 0), axis=2)
    route_cap = jnp.sum(jnp.where(matches, capacity[None, None, :], 0), axis=2)
    kept_mask = route_pos < route_cap
    slot_index = jnp.where(kept_mask, routes * slot_count + route_pos, -1)
    first_share = gate_num.astype(jnp.float32) / 64.0
    weights = jnp.where(kept_mask, jnp.stack([first_share, 1.0 - first_share], axis=1), 0.0)
    slot_ids = jnp.arange(expert_count * slot_count, dtype=jnp.int32)
    dispatch = jnp.any(slot_ids[:, None, None] == slot_index[None, :, :], axis=2)
    combine_hits = slot_ids[None, :, None] == slot_index[:, None, :]
    combine = jnp.sum(jnp.where(combine_hits, weights[:, None, :], 0.0), axis=2)
    return dispatch.astype(jnp.bfloat16), combine.astype(jnp.bfloat16)


def ring(value):
    count, low = lax.axis_size(CIRCLE), lax.axis_size("mp")

    def rank(y, core):
        return (y // low * 2 + core) * low + y % low

    pairs = [(rank(y, 0), rank((y + 1) % count, 0)) for y in range(count)]
    pairs += [(rank(y, 1), rank((y - 1) % count, 1)) for y in range(count)]
    return lax.ppermute(value, ("yh", "core", "mp"), pairs)


def swap(value):
    return lax.ppermute(value, "core", [(0, 1), (1, 0)])


def add(a, b):
    return (a.astype(jnp.float32) + b.astype(jnp.float32)).astype(jnp.bfloat16)


def per_device(tokens, routes, gate_num, capacity, w_up, w_down):
    expert_count = capacity.shape[0]
    token_count, width = tokens.shape
    features = w_up.shape[0]
    slot_count = min(token_count, 3 * token_count // expert_count)
    half = lax.axis_size(CIRCLE) // 2
    place = jnp.stack([lax.axis_index(CIRCLE), 1 - 2 * lax.axis_index("core")])
    place, routes = lax.optimization_barrier((place.astype(jnp.int32), routes))
    up = w_up.T
    weights = (up, swap(up), w_down, swap(w_down))
    dispatch, combine = routing(routes, gate_num, capacity, slot_count)

    rows = jnp.dot(dispatch, tokens, preferred_element_type=jnp.float32).astype(jnp.bfloat16)
    arrived = lax.all_to_all(
        rows.reshape(expert_count, slot_count, width), "z", 0, 0, tiled=True
    )
    mine = [arrived.reshape(expert_count * slot_count, width)]
    other = [swap(mine[0])]
    crossed = []
    for step in range(1, half + 1):
        mine.append(ring(mine[-1]))
        if step < half:
            other.append(ring(other[-1]))
            crossed.append(swap(other[-1]))

    *own, given = ffn(place, mine + crossed, weights, features)

    taken = swap(given)
    mine_sum = ring(own[half])
    other_sum = ring(taken[half - 2])
    for step in range(half - 1, 0, -1):
        mine_sum = ring(add(own[step], mine_sum))
        if step > 1:
            other_sum = ring(add(taken[step - 2], other_sum))
    crossed_sum = swap(other_sum)

    total = own[0].astype(jnp.float32) + mine_sum.astype(jnp.float32)
    total = (total + crossed_sum.astype(jnp.float32)).astype(jnp.bfloat16)
    back = lax.all_to_all(
        total.reshape(expert_count, slot_count, width), "z", 0, 0, tiled=True
    )
    mixed = jnp.dot(
        combine,
        back.reshape(expert_count * slot_count, width),
        preferred_element_type=jnp.float32,
    )
    return mixed.astype(jnp.bfloat16)


def solution(mesh):
    sizes = dict(mesh.shape)
    group = sizes["expert"] // EXPERTS
    devices = mesh.devices.reshape(sizes["dp"], EXPERTS, group // 2, 2, sizes["mp"])
    fine = Mesh(devices, ("dp", "z", "yh", "core", "mp"))
    expert = ("z", "yh", "core")
    return jax.shard_map(
        per_device,
        mesh=fine,
        in_specs=(
            P(("dp", *expert), "mp"),
            P(("dp", *expert), None),
            P(("dp", *expert)),
            P(),
            P(None, (*expert, "mp")),
            P((*expert, "mp"), None),
        ),
        out_specs=P(("dp", *expert), "mp"),
        check_vma=False,
    )
```

```python
import jax
import jax.numpy as jnp
from jax import lax
from jax.experimental import pallas as pl
from jax.experimental.pallas import tpu as pltpu
from jax.sharding import Mesh, PartitionSpec as P


EXPERTS = 8
CIRCLE = ("yh", "mp")
EARLY = (0, -1, -2, -3, 1, 2)
LATE = (-4, 3)


def spot(place_ref, offset, rows, width, features):
    chunks = features // width
    source = lax.rem(place_ref[0] + place_ref[1] * offset + 2 * chunks, 2 * chunks)
    row = pl.multiple_of(lax.div(source, chunks) * rows, rows)
    col = pl.multiple_of(lax.rem(source, chunks) * width, width)
    return lax.div(source, chunks), pl.ds(row, rows), pl.ds(col, width)


def projected(x, up):
    return lax.dot_general(x, up, (((1,), (1,)), ((), ())), preferred_element_type=jnp.float32)


def early_body(place_ref, *refs):
    count = len(EARLY)
    x_refs, stored, kept = refs[:count], refs[count : count + 4], refs[count + 6 : count + 10]
    sums, sems = refs[count + 4 : count + 6], refs[-1]
    copies = [
        pltpu.make_async_copy(src, dst, sems.at[i])
        for i, (src, dst) in enumerate(zip(stored, kept))
    ]
    for copy in copies:
        copy.start()
    for total in sums:
        total[...] = jnp.zeros_like(total)
    for copy in copies[:2]:
        copy.wait()
    for x_ref, offset in zip(x_refs, EARLY):
        _, rows, cols = spot(place_ref, offset, *x_ref.shape, kept[0].shape[1])
        for total, up in zip(sums, kept[:2]):
            total[rows, :] += projected(x_ref[...], up[:, cols])
    for copy in copies[2:]:
        copy.wait()


def send_down(place_ref, offset, hidden, down, shape):
    _, rows, cols = spot(place_ref, offset, *shape, down[0].shape[1])
    total = jnp.dot(hidden[0][rows, :], down[0][:, cols], preferred_element_type=jnp.float32)
    total += jnp.dot(hidden[1][rows, :], down[1][:, cols], preferred_element_type=jnp.float32)
    return total.astype(jnp.bfloat16)


def middle_body(place_ref, *refs):
    sums, x_refs, up, down = refs[:2], refs[2:4], refs[4:6], refs[6:8]
    first, given, *hidden = refs[8:]
    rows, width = shape = first.shape
    for total, up_ref, out in zip(sums, up, hidden):
        late = []
        for x_ref, offset in zip(x_refs, LATE):
            group, _, cols = spot(place_ref, offset, *shape, up_ref.shape[1])
            late.append((group, projected(x_ref[...], up_ref[:, cols])))
        for g in range(2):
            acc = total[g * rows : (g + 1) * rows, :]
            for group, value in late:
                acc = acc + jnp.where(group == g, value, 0.0)
            silu = acc / (1.0 + jnp.exp(-acc))
            out[g * rows : (g + 1) * rows, :] = silu.astype(jnp.bfloat16)
    first[...] = send_down(place_ref, 4, hidden, down, shape)
    for j in reversed(range(given.shape[0])):
        given[j] = send_down(place_ref, -1 - j, hidden, down, shape)


def last_body(place_ref, *refs):
    hidden, down, outs = refs[:2], refs[2:4], refs[4:]
    for j in reversed(range(len(outs))):
        outs[j][...] = send_down(place_ref, j, hidden, down, outs[j].shape)


def kernel(body, place, on_chip, stored, shapes, sems=0):
    vmem = pl.BlockSpec(memory_space=pltpu.VMEM)
    hbm = pl.BlockSpec(memory_space=pltpu.HBM)
    return pl.pallas_call(
        body,
        in_specs=[pl.BlockSpec(memory_space=pltpu.SMEM)]
        + [vmem] * len(on_chip)
        + [hbm] * len(stored),
        out_specs=[vmem] * len(shapes),
        out_shape=[jax.ShapeDtypeStruct(*shape) for shape in shapes],
        scratch_shapes=[pltpu.SemaphoreType.DMA((sems,))] if sems else [],
        compiler_params=pltpu.CompilerParams(vmem_limit_bytes=20 << 20),
    )(place, *on_chip, *stored)


def routing(routes, gate_num, capacity, slot_count):
    token_count = routes.shape[0]
    expert_count = capacity.shape[0]
    expert_ids = jnp.arange(expert_count, dtype=jnp.int32)
    matches = routes[:, :, None] == expert_ids[None, None, :]
    named_count = matches.sum(axis=1).astype(jnp.bfloat16)
    token_ids = jnp.arange(token_count, dtype=jnp.int32)
    lower_mask = (token_ids[:, None] > token_ids[None, :]).astype(jnp.bfloat16)
    positions = jnp.dot(
        lower_mask, named_count, preferred_element_type=jnp.float32
    ).astype(jnp.int32)
    route_pos = jnp.sum(jnp.where(matches, positions[:, None, :], 0), axis=2)
    route_cap = jnp.sum(jnp.where(matches, capacity[None, None, :], 0), axis=2)
    kept_mask = route_pos < route_cap
    slot_index = jnp.where(kept_mask, routes * slot_count + route_pos, -1)
    first_share = gate_num.astype(jnp.float32) / 64.0
    weights = jnp.where(kept_mask, jnp.stack([first_share, 1.0 - first_share], axis=1), 0.0)
    slot_ids = jnp.arange(expert_count * slot_count, dtype=jnp.int32)
    dispatch = jnp.any(slot_ids[:, None, None] == slot_index[None, :, :], axis=2)
    combine_hits = slot_ids[None, :, None] == slot_index[:, None, :]
    combine = jnp.sum(jnp.where(combine_hits, weights[:, None, :], 0.0), axis=2)
    return dispatch.astype(jnp.bfloat16), combine.astype(jnp.bfloat16)


def ring(value):
    count, low = lax.axis_size(CIRCLE), lax.axis_size("mp")

    def rank(y, core):
        return (y // low * 2 + core) * low + y % low

    pairs = [(rank(y, 0), rank((y + 1) % count, 0)) for y in range(count)]
    pairs += [(rank(y, 1), rank((y - 1) % count, 1)) for y in range(count)]
    return lax.ppermute(value, ("yh", "core", "mp"), pairs)


def swap(value):
    return lax.ppermute(value, "core", [(0, 1), (1, 0)])


def add(a, b):
    return (a.astype(jnp.float32) + b.astype(jnp.float32)).astype(jnp.bfloat16)


def per_device(tokens, routes, gate_num, capacity, w_up, w_down):
    expert_count = capacity.shape[0]
    token_count, width = tokens.shape
    slot_count = min(token_count, 3 * token_count // expert_count)
    half = lax.axis_size(CIRCLE) // 2
    place = jnp.stack([lax.axis_index(CIRCLE), 1 - 2 * lax.axis_index("core")])
    place, routes = lax.optimization_barrier((place.astype(jnp.int32), routes))
    up = w_up.T
    weights = (up, swap(up), w_down, swap(w_down))
    hidden_width = up.shape[0]
    dispatch, combine = routing(routes, gate_num, capacity, slot_count)

    rows = jnp.dot(dispatch, tokens, preferred_element_type=jnp.float32).astype(jnp.bfloat16)
    arrived = lax.all_to_all(rows.reshape(expert_count, slot_count, width), "z", 0, 0, tiled=True)
    mine = [arrived.reshape(expert_count * slot_count, width)]
    other = [swap(mine[0])]
    crossed = []
    for step in range(1, half + 1):
        mine.append(ring(mine[-1]))
        if step < half:
            other.append(ring(other[-1]))
            crossed.append(swap(other[-1]))

    chunk = (mine[0].shape, jnp.bfloat16)
    total_rows = 2 * mine[0].shape[0]
    sums = [((total_rows, hidden_width), jnp.float32)] * 2
    kept = [(weight.shape, weight.dtype) for weight in weights]
    sum_a, sum_b, *kept = kernel(
        early_body, place, mine[:half] + crossed[:2], weights, sums + kept, 4
    )
    first, given, *hidden = kernel(
        middle_body,
        place,
        [sum_a, sum_b, mine[half], crossed[2], *kept],
        [],
        [chunk, ((half - 1, *chunk[0]), chunk[1])]
        + [((total_rows, hidden_width), jnp.bfloat16)] * 2,
    )
    own = kernel(last_body, place, [*hidden, *kept[2:]], [], [chunk] * half)
    own = [*own, first]

    taken = swap(given)
    mine_sum = ring(own[half])
    other_sum = ring(taken[half - 2])
    for step in range(half - 1, 0, -1):
        mine_sum = ring(add(own[step], mine_sum))
        if step > 1:
            other_sum = ring(add(taken[step - 2], other_sum))
    crossed_sum = swap(other_sum)

    total = own[0].astype(jnp.float32) + mine_sum.astype(jnp.float32)
    total = (total + crossed_sum.astype(jnp.float32)).astype(jnp.bfloat16)
    back = lax.all_to_all(
        total.reshape(expert_count, slot_count, width), "z", 0, 0, tiled=True
    )
    mixed = jnp.dot(
        combine,
        back.reshape(expert_count * slot_count, width),
        preferred_element_type=jnp.float32,
    )
    return mixed.astype(jnp.bfloat16)


def solution(mesh):
    sizes = dict(mesh.shape)
    group = sizes["expert"] // EXPERTS
    devices = mesh.devices.reshape(sizes["dp"], EXPERTS, group // 2, 2, sizes["mp"])
    fine = Mesh(devices, ("dp", "z", "yh", "core", "mp"))
    expert = ("z", "yh", "core")
    return jax.shard_map(
        per_device,
        mesh=fine,
        in_specs=(
            P(("dp", *expert), "mp"),
            P(("dp", *expert), None),
            P(("dp", *expert)),
            P(),
            P(None, (*expert, "mp")),
            P((*expert, "mp"), None),
        ),
        out_specs=P(("dp", *expert), "mp"),
        check_vma=False,
    )
```

```python
import functools

import jax
import jax.numpy as jnp
from jax import lax
from jax.experimental import pallas as pl
from jax.experimental.pallas import tpu as pltpu
from jax.sharding import Mesh, PartitionSpec as P


EXPERTS = 8
CIRCLE = ("yh", "mp")
EARLY = ((0, -1), (-2, 1), (-3, 2))
LATE = (-4, 3)


def spot(place_ref, offset, rows, width, features):
    chunks = features // width
    source = lax.rem(place_ref[0] + place_ref[1] * offset + 2 * chunks, 2 * chunks)
    row = pl.multiple_of(lax.div(source, chunks) * rows, rows)
    col = pl.multiple_of(lax.rem(source, chunks) * width, width)
    return lax.div(source, chunks), pl.ds(row, rows), pl.ds(col, width)


def projected(x, up):
    return lax.dot_general(x, up, (((1,), (1,)), ((), ())), preferred_element_type=jnp.float32)


def early_body(offsets, place_ref, *refs):
    refs = list(refs)
    first, sems = offsets is EARLY[0], refs.pop() if offsets is not EARLY[2] else None
    x_refs = [refs.pop(0) for _ in offsets]
    before = [] if first else [refs.pop(0) for _ in range(2)]
    up = [] if first else [refs.pop(0) for _ in range(2)]
    stored = [] if sems is None else [refs.pop(0) for _ in range(2)]
    sums, kept = refs[:2], refs[2:]
    copies = [
        pltpu.make_async_copy(src, dst, sems.at[i])
        for i, (src, dst) in enumerate(zip(stored, kept))
    ]
    for copy in copies:
        copy.start()
    for i, total in enumerate(sums):
        total[...] = jnp.zeros_like(total) if first else before[i][...]
    if first:
        up = kept
        for copy in copies:
            copy.wait()
    for x_ref, offset in zip(x_refs, offsets):
        _, rows, cols = spot(place_ref, offset, *x_ref.shape, up[0].shape[1])
        for total, up_ref in zip(sums, up):
            total[rows, :] += projected(x_ref[...], up_ref[:, cols])
    if not first:
        for copy in copies:
            copy.wait()


def send_down(place_ref, offset, hidden, down, shape):
    _, rows, cols = spot(place_ref, offset, *shape, down[0].shape[1])
    total = jnp.dot(hidden[0][rows, :], down[0][:, cols], preferred_element_type=jnp.float32)
    total += jnp.dot(hidden[1][rows, :], down[1][:, cols], preferred_element_type=jnp.float32)
    return total.astype(jnp.bfloat16)


def middle_body(place_ref, *refs):
    sums, x_refs, up, down = refs[:2], refs[2:4], refs[4:6], refs[6:8]
    first, given, *hidden = refs[8:]
    rows, width = shape = first.shape
    for total, up_ref, out in zip(sums, up, hidden):
        late = []
        for x_ref, offset in zip(x_refs, LATE):
            group, _, cols = spot(place_ref, offset, *shape, up_ref.shape[1])
            late.append((group, projected(x_ref[...], up_ref[:, cols])))
        for g in range(2):
            acc = total[g * rows : (g + 1) * rows, :]
            for group, value in late:
                acc = acc + jnp.where(group == g, value, 0.0)
            silu = acc / (1.0 + jnp.exp(-acc))
            out[g * rows : (g + 1) * rows, :] = silu.astype(jnp.bfloat16)
    first[...] = send_down(place_ref, 4, hidden, down, shape)
    for j in reversed(range(given.shape[0])):
        given[j] = send_down(place_ref, -1 - j, hidden, down, shape)


def last_body(place_ref, *refs):
    hidden, down, outs = refs[:2], refs[2:4], refs[4:]
    for j in reversed(range(len(outs))):
        outs[j][...] = send_down(place_ref, j, hidden, down, outs[j].shape)


def kernel(body, place, on_chip, stored, shapes, sems=0):
    vmem = pl.BlockSpec(memory_space=pltpu.VMEM)
    hbm = pl.BlockSpec(memory_space=pltpu.HBM)
    return pl.pallas_call(
        body,
        in_specs=[pl.BlockSpec(memory_space=pltpu.SMEM)]
        + [vmem] * len(on_chip)
        + [hbm] * len(stored),
        out_specs=[vmem] * len(shapes),
        out_shape=[jax.ShapeDtypeStruct(*shape) for shape in shapes],
        scratch_shapes=[pltpu.SemaphoreType.DMA((sems,))] if sems else [],
        compiler_params=pltpu.CompilerParams(vmem_limit_bytes=20 << 20),
    )(place, *on_chip, *stored)


def routing(routes, gate_num, capacity, slot_count):
    token_count = routes.shape[0]
    expert_count = capacity.shape[0]
    expert_ids = jnp.arange(expert_count, dtype=jnp.int32)
    matches = routes[:, :, None] == expert_ids[None, None, :]
    named_count = matches.sum(axis=1).astype(jnp.bfloat16)
    token_ids = jnp.arange(token_count, dtype=jnp.int32)
    lower_mask = (token_ids[:, None] > token_ids[None, :]).astype(jnp.bfloat16)
    positions = jnp.dot(
        lower_mask, named_count, preferred_element_type=jnp.float32
    ).astype(jnp.int32)
    route_pos = jnp.sum(jnp.where(matches, positions[:, None, :], 0), axis=2)
    route_cap = jnp.sum(jnp.where(matches, capacity[None, None, :], 0), axis=2)
    kept_mask = route_pos < route_cap
    slot_index = jnp.where(kept_mask, routes * slot_count + route_pos, -1)
    first_share = gate_num.astype(jnp.float32) / 64.0
    weights = jnp.where(kept_mask, jnp.stack([first_share, 1.0 - first_share], axis=1), 0.0)
    slot_ids = jnp.arange(expert_count * slot_count, dtype=jnp.int32)
    dispatch = jnp.any(slot_ids[:, None, None] == slot_index[None, :, :], axis=2)
    combine_hits = slot_ids[None, :, None] == slot_index[:, None, :]
    combine = jnp.sum(jnp.where(combine_hits, weights[:, None, :], 0.0), axis=2)
    return dispatch.astype(jnp.bfloat16), combine.astype(jnp.bfloat16)


def ring(value):
    count, low = lax.axis_size(CIRCLE), lax.axis_size("mp")

    def rank(y, core):
        return (y // low * 2 + core) * low + y % low

    pairs = [(rank(y, 0), rank((y + 1) % count, 0)) for y in range(count)]
    pairs += [(rank(y, 1), rank((y - 1) % count, 1)) for y in range(count)]
    return lax.ppermute(value, ("yh", "core", "mp"), pairs)


def swap(value):
    return lax.ppermute(value, "core", [(0, 1), (1, 0)])


def add(a, b):
    return (a.astype(jnp.float32) + b.astype(jnp.float32)).astype(jnp.bfloat16)


def per_device(tokens, routes, gate_num, capacity, w_up, w_down):
    expert_count = capacity.shape[0]
    token_count, width = tokens.shape
    slot_count = min(token_count, 3 * token_count // expert_count)
    half = lax.axis_size(CIRCLE) // 2
    place = jnp.stack([lax.axis_index(CIRCLE), 1 - 2 * lax.axis_index("core")])
    place, routes = lax.optimization_barrier((place.astype(jnp.int32), routes))
    up = w_up.T
    weights = (up, swap(up), w_down, swap(w_down))
    hidden_width = up.shape[0]
    dispatch, combine = routing(routes, gate_num, capacity, slot_count)

    rows = jnp.dot(dispatch, tokens, preferred_element_type=jnp.float32).astype(jnp.bfloat16)
    arrived = lax.all_to_all(rows.reshape(expert_count, slot_count, width), "z", 0, 0, tiled=True)
    mine = [arrived.reshape(expert_count * slot_count, width)]
    other = [swap(mine[0])]
    crossed = []
    for step in range(1, half + 1):
        mine.append(ring(mine[-1]))
        if step < half:
            other.append(ring(other[-1]))
            crossed.append(swap(other[-1]))

    chunk = (mine[0].shape, jnp.bfloat16)
    total_rows = 2 * mine[0].shape[0]
    sums = [((total_rows, hidden_width), jnp.float32)] * 2
    kept = [(weight.shape, weight.dtype) for weight in weights]
    *sum_refs, up_a, up_b = kernel(
        functools.partial(early_body, EARLY[0]), place, mine[:2], weights[:2], sums + kept[:2], 2
    )
    *sum_refs, down_a, down_b = kernel(
        functools.partial(early_body, EARLY[1]),
        place,
        [mine[2], crossed[0], *sum_refs, up_a, up_b],
        weights[2:],
        sums + kept[2:],
        2,
    )
    sum_refs = kernel(
        functools.partial(early_body, EARLY[2]),
        place,
        [mine[3], crossed[1], *sum_refs, up_a, up_b],
        [],
        sums,
    )
    first, given, *hidden = kernel(
        middle_body,
        place,
        [*sum_refs, mine[half], crossed[2], up_a, up_b, down_a, down_b],
        [],
        [chunk, ((half - 1, *chunk[0]), chunk[1])]
        + [((total_rows, hidden_width), jnp.bfloat16)] * 2,
    )
    own = kernel(last_body, place, [*hidden, down_a, down_b], [], [chunk] * half)
    own = [*own, first]

    taken = swap(given)
    mine_sum = ring(own[half])
    other_sum = ring(taken[half - 2])
    for step in range(half - 1, 0, -1):
        mine_sum = ring(add(own[step], mine_sum))
        if step > 1:
            other_sum = ring(add(taken[step - 2], other_sum))
    crossed_sum = swap(other_sum)

    total = own[0].astype(jnp.float32) + mine_sum.astype(jnp.float32)
    total = (total + crossed_sum.astype(jnp.float32)).astype(jnp.bfloat16)
    back = lax.all_to_all(
        total.reshape(expert_count, slot_count, width), "z", 0, 0, tiled=True
    )
    mixed = jnp.dot(
        combine,
        back.reshape(expert_count * slot_count, width),
        preferred_element_type=jnp.float32,
    )
    return mixed.astype(jnp.bfloat16)


def solution(mesh):
    sizes = dict(mesh.shape)
    group = sizes["expert"] // EXPERTS
    devices = mesh.devices.reshape(sizes["dp"], EXPERTS, group // 2, 2, sizes["mp"])
    fine = Mesh(devices, ("dp", "z", "yh", "core", "mp"))
    expert = ("z", "yh", "core")
    return jax.shard_map(
        per_device,
        mesh=fine,
        in_specs=(
            P(("dp", *expert), "mp"),
            P(("dp", *expert), None),
            P(("dp", *expert)),
            P(),
            P(None, (*expert, "mp")),
            P((*expert, "mp"), None),
        ),
        out_specs=P(("dp", *expert), "mp"),
        check_vma=False,
    )
```

```python
import functools

import jax
import jax.numpy as jnp
from jax import lax
from jax.experimental import pallas as pl
from jax.experimental.pallas import tpu as pltpu
from jax.sharding import Mesh, PartitionSpec as P


EXPERTS = 8
CIRCLE = ("yh", "mp")
EARLY = ((0, -1), (-2,), (1, -3))
LATE = (-4, 2, 3)


def spot(place_ref, offset, rows, width, features):
    chunks = features // width
    source = lax.rem(place_ref[0] + place_ref[1] * offset + 2 * chunks, 2 * chunks)
    row = pl.multiple_of(lax.div(source, chunks) * rows, rows)
    col = pl.multiple_of(lax.rem(source, chunks) * width, width)
    return lax.div(source, chunks), pl.ds(row, rows), pl.ds(col, width)


def projected(x, up):
    return lax.dot_general(x, up, (((1,), (1,)), ((), ())), preferred_element_type=jnp.float32)


def early_body(offsets, place_ref, *refs):
    refs = list(refs)
    first, sems = offsets is EARLY[0], refs.pop() if offsets is not EARLY[2] else None
    x_refs = [refs.pop(0) for _ in offsets]
    before = [] if first else [refs.pop(0) for _ in range(2)]
    up = [] if first else [refs.pop(0) for _ in range(2)]
    stored = [] if sems is None else [refs.pop(0) for _ in range(2)]
    sums, kept = refs[:2], refs[2:]
    copies = [
        pltpu.make_async_copy(src, dst, sems.at[i])
        for i, (src, dst) in enumerate(zip(stored, kept))
    ]
    for copy in copies:
        copy.start()
    for i, total in enumerate(sums):
        total[...] = jnp.zeros_like(total) if first else before[i][...]
    if first:
        up = kept
        for copy in copies:
            copy.wait()
    for x_ref, offset in zip(x_refs, offsets):
        _, rows, cols = spot(place_ref, offset, *x_ref.shape, up[0].shape[1])
        for total, up_ref in zip(sums, up):
            total[rows, :] += projected(x_ref[...], up_ref[:, cols])
    if not first:
        for copy in copies:
            copy.wait()


def send_down(place_ref, offset, hidden, down, shape):
    _, rows, cols = spot(place_ref, offset, *shape, down[0].shape[1])
    total = jnp.dot(hidden[0][rows, :], down[0][:, cols], preferred_element_type=jnp.float32)
    total += jnp.dot(hidden[1][rows, :], down[1][:, cols], preferred_element_type=jnp.float32)
    return total.astype(jnp.bfloat16)


def middle_body(place_ref, *refs):
    sums, x_refs, refs = refs[:2], refs[2 : 2 + len(LATE)], refs[2 + len(LATE) :]
    up, down, first, hidden = refs[:2], refs[2:4], refs[4], refs[5:]
    rows, width = shape = first.shape
    for total, up_ref, out in zip(sums, up, hidden):
        late = []
        for x_ref, offset in zip(x_refs, LATE):
            group, _, cols = spot(place_ref, offset, *shape, up_ref.shape[1])
            late.append((group, projected(x_ref[...], up_ref[:, cols])))
        for g in range(2):
            acc = total[g * rows : (g + 1) * rows, :]
            for group, value in late:
                acc = acc + jnp.where(group == g, value, 0.0)
            silu = acc / (1.0 + jnp.exp(-acc))
            out[g * rows : (g + 1) * rows, :] = silu.astype(jnp.bfloat16)
    first[...] = send_down(place_ref, 4, hidden, down, shape)


def given_body(place_ref, *refs):
    hidden, down, given = refs[:2], refs[2:4], refs[4]
    for j in reversed(range(given.shape[0])):
        given[j] = send_down(place_ref, -1 - j, hidden, down, given.shape[1:])


def last_body(place_ref, *refs):
    hidden, down, outs = refs[:2], refs[2:4], refs[4:]
    for j in reversed(range(len(outs))):
        outs[j][...] = send_down(place_ref, j, hidden, down, outs[j].shape)


def kernel(body, place, on_chip, stored, shapes, sems=0):
    vmem = pl.BlockSpec(memory_space=pltpu.VMEM)
    hbm = pl.BlockSpec(memory_space=pltpu.HBM)
    return pl.pallas_call(
        body,
        in_specs=[pl.BlockSpec(memory_space=pltpu.SMEM)]
        + [vmem] * len(on_chip)
        + [hbm] * len(stored),
        out_specs=[vmem] * len(shapes),
        out_shape=[jax.ShapeDtypeStruct(*shape) for shape in shapes],
        scratch_shapes=[pltpu.SemaphoreType.DMA((sems,))] if sems else [],
        compiler_params=pltpu.CompilerParams(vmem_limit_bytes=20 << 20),
    )(place, *on_chip, *stored)


def routing(routes, gate_num, capacity, slot_count):
    token_count = routes.shape[0]
    expert_count = capacity.shape[0]
    expert_ids = jnp.arange(expert_count, dtype=jnp.int32)
    matches = routes[:, :, None] == expert_ids[None, None, :]
    named_count = matches.sum(axis=1).astype(jnp.bfloat16)
    token_ids = jnp.arange(token_count, dtype=jnp.int32)
    lower_mask = (token_ids[:, None] > token_ids[None, :]).astype(jnp.bfloat16)
    positions = jnp.dot(
        lower_mask, named_count, preferred_element_type=jnp.float32
    ).astype(jnp.int32)
    route_pos = jnp.sum(jnp.where(matches, positions[:, None, :], 0), axis=2)
    route_cap = jnp.sum(jnp.where(matches, capacity[None, None, :], 0), axis=2)
    kept_mask = route_pos < route_cap
    slot_index = jnp.where(kept_mask, routes * slot_count + route_pos, -1)
    first_share = gate_num.astype(jnp.float32) / 64.0
    weights = jnp.where(kept_mask, jnp.stack([first_share, 1.0 - first_share], axis=1), 0.0)
    slot_ids = jnp.arange(expert_count * slot_count, dtype=jnp.int32)
    dispatch = jnp.any(slot_ids[:, None, None] == slot_index[None, :, :], axis=2)
    combine_hits = slot_ids[None, :, None] == slot_index[:, None, :]
    combine = jnp.sum(jnp.where(combine_hits, weights[:, None, :], 0.0), axis=2)
    return dispatch.astype(jnp.bfloat16), combine.astype(jnp.bfloat16)


def ring(value):
    count, low = lax.axis_size(CIRCLE), lax.axis_size("mp")

    def rank(y, core):
        return (y // low * 2 + core) * low + y % low

    pairs = [(rank(y, 0), rank((y + 1) % count, 0)) for y in range(count)]
    pairs += [(rank(y, 1), rank((y - 1) % count, 1)) for y in range(count)]
    return lax.ppermute(value, ("yh", "core", "mp"), pairs)


def swap(value):
    return lax.ppermute(value, "core", [(0, 1), (1, 0)])


def add(a, b):
    return (a.astype(jnp.float32) + b.astype(jnp.float32)).astype(jnp.bfloat16)


def per_device(tokens, routes, gate_num, capacity, w_up, w_down):
    expert_count = capacity.shape[0]
    token_count, width = tokens.shape
    slot_count = min(token_count, 3 * token_count // expert_count)
    half = lax.axis_size(CIRCLE) // 2
    place = jnp.stack([lax.axis_index(CIRCLE), 1 - 2 * lax.axis_index("core")])
    place, routes = lax.optimization_barrier((place.astype(jnp.int32), routes))
    up = w_up.T
    weights = (up, swap(up), w_down, swap(w_down))
    hidden_width = up.shape[0]
    dispatch, combine = routing(routes, gate_num, capacity, slot_count)

    rows = jnp.dot(dispatch, tokens, preferred_element_type=jnp.float32).astype(jnp.bfloat16)
    arrived = lax.all_to_all(rows.reshape(expert_count, slot_count, width), "z", 0, 0, tiled=True)
    mine = [arrived.reshape(expert_count * slot_count, width)]
    other = [swap(mine[0])]
    crossed = []
    for step in range(1, half + 1):
        mine.append(ring(mine[-1]))
        if step < half:
            other.append(ring(other[-1]))
            crossed.append(swap(other[-1]))

    chunk = (mine[0].shape, jnp.bfloat16)
    total_rows = 2 * mine[0].shape[0]
    sums = [((total_rows, hidden_width), jnp.float32)] * 2
    kept = [(weight.shape, weight.dtype) for weight in weights]
    *sum_refs, up_a, up_b = kernel(
        functools.partial(early_body, EARLY[0]), place, mine[:2], weights[:2], sums + kept[:2], 2
    )
    *sum_refs, down_a, down_b = kernel(
        functools.partial(early_body, EARLY[1]),
        place,
        [mine[2], *sum_refs, up_a, up_b],
        weights[2:],
        sums + kept[2:],
        2,
    )
    sum_refs = kernel(
        functools.partial(early_body, EARLY[2]),
        place,
        [crossed[0], mine[3], *sum_refs, up_a, up_b],
        [],
        sums,
    )
    first, *hidden = kernel(
        middle_body,
        place,
        [*sum_refs, mine[half], *crossed[1:], up_a, up_b, down_a, down_b],
        [],
        [chunk] + [((total_rows, hidden_width), jnp.bfloat16)] * 2,
    )
    given_shape = ((half - 1, *chunk[0]), chunk[1])
    (given,) = kernel(given_body, place, [*hidden, down_a, down_b], [], [given_shape])
    own = kernel(last_body, place, [*hidden, down_a, down_b], [], [chunk] * half)
    own = [*own, first]

    taken = swap(given)
    mine_sum = ring(own[half])
    other_sum = ring(taken[half - 2])
    for step in range(half - 1, 0, -1):
        mine_sum = ring(add(own[step], mine_sum))
        if step > 1:
            other_sum = ring(add(taken[step - 2], other_sum))
    crossed_sum = swap(other_sum)

    total = own[0].astype(jnp.float32) + mine_sum.astype(jnp.float32)
    total = (total + crossed_sum.astype(jnp.float32)).astype(jnp.bfloat16)
    back = lax.all_to_all(
        total.reshape(expert_count, slot_count, width), "z", 0, 0, tiled=True
    )
    mixed = jnp.dot(
        combine,
        back.reshape(expert_count * slot_count, width),
        preferred_element_type=jnp.float32,
    )
    return mixed.astype(jnp.bfloat16)


def solution(mesh):
    sizes = dict(mesh.shape)
    group = sizes["expert"] // EXPERTS
    devices = mesh.devices.reshape(sizes["dp"], EXPERTS, group // 2, 2, sizes["mp"])
    fine = Mesh(devices, ("dp", "z", "yh", "core", "mp"))
    expert = ("z", "yh", "core")
    return jax.shard_map(
        per_device,
        mesh=fine,
        in_specs=(
            P(("dp", *expert), "mp"),
            P(("dp", *expert), None),
            P(("dp", *expert)),
            P(),
            P(None, (*expert, "mp")),
            P((*expert, "mp"), None),
        ),
        out_specs=P(("dp", *expert), "mp"),
        check_vma=False,
    )
```

```python
import functools

import jax
import jax.numpy as jnp
from jax import lax
from jax.experimental import pallas as pl
from jax.experimental.pallas import tpu as pltpu
from jax.sharding import Mesh, PartitionSpec as P


EXPERTS = 8
CIRCLE = ("yh", "mp")
EARLY = ((0, -1), (-2,), (1, -3))
LATE = (-4, 2, 3)


def spot(place_ref, offset, rows, width, features):
    chunks = features // width
    source = lax.rem(place_ref[0] + place_ref[1] * offset + 2 * chunks, 2 * chunks)
    row = pl.multiple_of(lax.div(source, chunks) * rows, rows)
    col = pl.multiple_of(lax.rem(source, chunks) * width, width)
    return lax.div(source, chunks), pl.ds(row, rows), pl.ds(col, width)


def projected(x, up):
    return lax.dot_general(x, up, (((1,), (1,)), ((), ())), preferred_element_type=jnp.float32)


def early_body(offsets, place_ref, *refs):
    refs = list(refs)
    first, sems = offsets is EARLY[0], refs.pop() if offsets is not EARLY[2] else None
    x_refs = [refs.pop(0) for _ in offsets]
    before = [] if first else [refs.pop(0) for _ in range(2)]
    up = [] if first else [refs.pop(0) for _ in range(2)]
    stored = [] if sems is None else [refs.pop(0) for _ in range(2)]
    sums, kept = refs[:2], refs[2:]
    copies = [
        pltpu.make_async_copy(src, dst, sems.at[i])
        for i, (src, dst) in enumerate(zip(stored, kept))
    ]
    for copy in copies:
        copy.start()
    for i, total in enumerate(sums):
        total[...] = jnp.zeros_like(total) if first else before[i][...]
    if first:
        up = kept
        for copy in copies:
            copy.wait()
    for x_ref, offset in zip(x_refs, offsets):
        _, rows, cols = spot(place_ref, offset, *x_ref.shape, up[0].shape[1])
        for total, up_ref in zip(sums, up):
            total[rows, :] += projected(x_ref[...], up_ref[:, cols])
    if not first:
        for copy in copies:
            copy.wait()


def send_down(place_ref, offset, hidden, down, shape):
    _, rows, cols = spot(place_ref, offset, *shape, down[0].shape[1])
    total = jnp.dot(hidden[0][rows, :], down[0][:, cols], preferred_element_type=jnp.float32)
    total += jnp.dot(hidden[1][rows, :], down[1][:, cols], preferred_element_type=jnp.float32)
    return total.astype(jnp.bfloat16)


def middle_body(place_ref, *refs):
    sums, x_refs, refs = refs[:2], refs[2 : 2 + len(LATE)], refs[2 + len(LATE) :]
    up, down, (first, given, *hidden) = refs[:2], refs[2:4], refs[4:]
    rows, width = shape = first.shape
    for total, up_ref, out in zip(sums, up, hidden):
        late = []
        for x_ref, offset in zip(x_refs, LATE):
            group, _, cols = spot(place_ref, offset, *shape, up_ref.shape[1])
            late.append((group, projected(x_ref[...], up_ref[:, cols])))
        for g in range(2):
            acc = total[g * rows : (g + 1) * rows, :]
            for group, value in late:
                acc = acc + jnp.where(group == g, value, 0.0)
            silu = acc / (1.0 + jnp.exp(-acc))
            out[g * rows : (g + 1) * rows, :] = silu.astype(jnp.bfloat16)
    first[...] = send_down(place_ref, 4, hidden, down, shape)
    for j in reversed(range(given.shape[0])):
        given[j] = send_down(place_ref, -1 - j, hidden, down, shape)


def last_body(place_ref, *refs):
    hidden, down, outs = refs[:2], refs[2:4], refs[4:]
    for j in reversed(range(len(outs))):
        outs[j][...] = send_down(place_ref, j, hidden, down, outs[j].shape)


def kernel(body, place, on_chip, stored, shapes, sems=0):
    vmem = pl.BlockSpec(memory_space=pltpu.VMEM)
    hbm = pl.BlockSpec(memory_space=pltpu.HBM)
    return pl.pallas_call(
        body,
        in_specs=[pl.BlockSpec(memory_space=pltpu.SMEM)]
        + [vmem] * len(on_chip)
        + [hbm] * len(stored),
        out_specs=[vmem] * len(shapes),
        out_shape=[jax.ShapeDtypeStruct(*shape) for shape in shapes],
        scratch_shapes=[pltpu.SemaphoreType.DMA((sems,))] if sems else [],
        compiler_params=pltpu.CompilerParams(vmem_limit_bytes=20 << 20),
    )(place, *on_chip, *stored)


def routing(routes, gate_num, capacity, slot_count):
    token_count = routes.shape[0]
    expert_count = capacity.shape[0]
    expert_ids = jnp.arange(expert_count, dtype=jnp.int32)
    matches = routes[:, :, None] == expert_ids[None, None, :]
    named_count = matches.sum(axis=1).astype(jnp.bfloat16)
    token_ids = jnp.arange(token_count, dtype=jnp.int32)
    lower_mask = (token_ids[:, None] > token_ids[None, :]).astype(jnp.bfloat16)
    positions = jnp.dot(
        lower_mask, named_count, preferred_element_type=jnp.float32
    ).astype(jnp.int32)
    route_pos = jnp.sum(jnp.where(matches, positions[:, None, :], 0), axis=2)
    route_cap = jnp.sum(jnp.where(matches, capacity[None, None, :], 0), axis=2)
    kept_mask = route_pos < route_cap
    slot_index = jnp.where(kept_mask, routes * slot_count + route_pos, -1)
    first_share = gate_num.astype(jnp.float32) / 64.0
    weights = jnp.where(kept_mask, jnp.stack([first_share, 1.0 - first_share], axis=1), 0.0)
    slot_ids = jnp.arange(expert_count * slot_count, dtype=jnp.int32)
    dispatch = jnp.any(slot_ids[:, None, None] == slot_index[None, :, :], axis=2)
    combine_hits = slot_ids[None, :, None] == slot_index[:, None, :]
    combine = jnp.sum(jnp.where(combine_hits, weights[:, None, :], 0.0), axis=2)
    return dispatch.astype(jnp.bfloat16), combine.astype(jnp.bfloat16)


def ring(value):
    count, low = lax.axis_size(CIRCLE), lax.axis_size("mp")

    def rank(y, core):
        return (y // low * 2 + core) * low + y % low

    pairs = [(rank(y, 0), rank((y + 1) % count, 0)) for y in range(count)]
    pairs += [(rank(y, 1), rank((y - 1) % count, 1)) for y in range(count)]
    return lax.ppermute(value, ("yh", "core", "mp"), pairs)


def swap(value):
    return lax.ppermute(value, "core", [(0, 1), (1, 0)])


def add(a, b):
    return (a.astype(jnp.float32) + b.astype(jnp.float32)).astype(jnp.bfloat16)


def per_device(tokens, routes, gate_num, capacity, w_up, w_down):
    expert_count = capacity.shape[0]
    token_count, width = tokens.shape
    slot_count = min(token_count, 3 * token_count // expert_count)
    half = lax.axis_size(CIRCLE) // 2
    place = jnp.stack([lax.axis_index(CIRCLE), 1 - 2 * lax.axis_index("core")])
    place, routes = lax.optimization_barrier((place.astype(jnp.int32), routes))
    up = w_up.T
    weights = (up, swap(up), w_down, swap(w_down))
    hidden_width = up.shape[0]
    dispatch, combine = routing(routes, gate_num, capacity, slot_count)

    rows = jnp.dot(dispatch, tokens, preferred_element_type=jnp.float32).astype(jnp.bfloat16)
    arrived = lax.all_to_all(rows.reshape(expert_count, slot_count, width), "z", 0, 0, tiled=True)
    mine = [arrived.reshape(expert_count * slot_count, width)]
    other = [swap(mine[0])]
    crossed = []
    for step in range(1, half + 1):
        mine.append(ring(mine[-1]))
        if step < half:
            other.append(ring(other[-1]))
            crossed.append(swap(other[-1]))

    chunk = (mine[0].shape, jnp.bfloat16)
    total_rows = 2 * mine[0].shape[0]
    sums = [((total_rows, hidden_width), jnp.float32)] * 2
    kept = [(weight.shape, weight.dtype) for weight in weights]
    *sum_refs, up_a, up_b = kernel(
        functools.partial(early_body, EARLY[0]), place, mine[:2], weights[:2], sums + kept[:2], 2
    )
    *sum_refs, down_a, down_b = kernel(
        functools.partial(early_body, EARLY[1]),
        place,
        [mine[2], *sum_refs, up_a, up_b],
        weights[2:],
        sums + kept[2:],
        2,
    )
    sum_refs = kernel(
        functools.partial(early_body, EARLY[2]),
        place,
        [crossed[0], mine[3], *sum_refs, up_a, up_b],
        [],
        sums,
    )
    first, given, *hidden = kernel(
        middle_body,
        place,
        [*sum_refs, mine[half], *crossed[1:], up_a, up_b, down_a, down_b],
        [],
        [chunk, ((half - 1, *chunk[0]), chunk[1])]
        + [((total_rows, hidden_width), jnp.bfloat16)] * 2,
    )
    own = kernel(last_body, place, [*hidden, down_a, down_b], [], [chunk] * half)
    own = [*own, first]

    taken = swap(given)
    mine_sum = ring(own[half])
    other_sum = ring(taken[half - 2])
    for step in range(half - 1, 0, -1):
        mine_sum = ring(add(own[step], mine_sum))
        if step > 1:
            other_sum = ring(add(taken[step - 2], other_sum))
    crossed_sum = swap(other_sum)

    total = own[0].astype(jnp.float32) + mine_sum.astype(jnp.float32)
    total = (total + crossed_sum.astype(jnp.float32)).astype(jnp.bfloat16)
    back = lax.all_to_all(
        total.reshape(expert_count, slot_count, width), "z", 0, 0, tiled=True
    )
    mixed = jnp.dot(
        combine,
        back.reshape(expert_count * slot_count, width),
        preferred_element_type=jnp.float32,
    )
    return mixed.astype(jnp.bfloat16)


def solution(mesh):
    sizes = dict(mesh.shape)
    group = sizes["expert"] // EXPERTS
    devices = mesh.devices.reshape(sizes["dp"], EXPERTS, group // 2, 2, sizes["mp"])
    fine = Mesh(devices, ("dp", "z", "yh", "core", "mp"))
    expert = ("z", "yh", "core")
    return jax.shard_map(
        per_device,
        mesh=fine,
        in_specs=(
            P(("dp", *expert), "mp"),
            P(("dp", *expert), None),
            P(("dp", *expert)),
            P(),
            P(None, (*expert, "mp")),
            P((*expert, "mp"), None),
        ),
        out_specs=P(("dp", *expert), "mp"),
        check_vma=False,
    )
```

```python
import functools

import jax
import jax.numpy as jnp
from jax import lax
from jax.experimental import pallas as pl
from jax.experimental.pallas import tpu as pltpu
from jax.sharding import Mesh, PartitionSpec as P


EXPERTS = 8
CIRCLE = ("yh", "mp")
EARLY = ((0, -1), (-2,), (1, -3))
LATE = (-4, 2, 3)


def spot(place_ref, offset, rows, width, features):
    chunks = features // width
    source = lax.rem(place_ref[0] + place_ref[1] * offset + 2 * chunks, 2 * chunks)
    row = pl.multiple_of(lax.div(source, chunks) * rows, rows)
    col = pl.multiple_of(lax.rem(source, chunks) * width, width)
    return lax.div(source, chunks), pl.ds(row, rows), pl.ds(col, width)


def projected(x, up):
    return lax.dot_general(x, up, (((1,), (1,)), ((), ())), preferred_element_type=jnp.float32)


def early_body(offsets, place_ref, *refs):
    refs = list(refs)
    first, sems = offsets is EARLY[0], refs.pop() if offsets is not EARLY[2] else None
    x_refs = [refs.pop(0) for _ in offsets]
    before = [] if first else [refs.pop(0) for _ in range(2)]
    up = [] if first else [refs.pop(0) for _ in range(2)]
    stored = [] if sems is None else [refs.pop(0) for _ in range(2)]
    sums, kept = refs[:2], refs[2:]
    copies = [
        pltpu.make_async_copy(src, dst, sems.at[i])
        for i, (src, dst) in enumerate(zip(stored, kept))
    ]
    for copy in copies:
        copy.start()
    for i, total in enumerate(sums):
        total[...] = jnp.zeros_like(total) if first else before[i][...]
    if first:
        up = kept
        for copy in copies:
            copy.wait()
    for x_ref, offset in zip(x_refs, offsets):
        _, rows, cols = spot(place_ref, offset, *x_ref.shape, up[0].shape[1])
        for total, up_ref in zip(sums, up):
            total[rows, :] += projected(x_ref[...], up_ref[:, cols])
    if not first:
        for copy in copies:
            copy.wait()


def send_down(place_ref, offset, hidden, down, shape):
    _, rows, cols = spot(place_ref, offset, *shape, down[0].shape[1])
    total = jnp.dot(hidden[0][rows, :], down[0][:, cols], preferred_element_type=jnp.float32)
    total += jnp.dot(hidden[1][rows, :], down[1][:, cols], preferred_element_type=jnp.float32)
    return total.astype(jnp.bfloat16)


def middle_body(place_ref, *refs):
    sums, x_refs, refs = refs[:2], refs[2 : 2 + len(LATE)], refs[2 + len(LATE) :]
    up, down, (first, given, *hidden) = refs[:2], refs[2:4], refs[4:]
    rows, width = shape = first.shape
    for total, up_ref, out in zip(sums, up, hidden):
        late = []
        for x_ref, offset in zip(x_refs, LATE):
            group, _, cols = spot(place_ref, offset, *shape, up_ref.shape[1])
            late.append((group, projected(x_ref[...], up_ref[:, cols])))
        for g in range(2):
            acc = total[g * rows : (g + 1) * rows, :]
            for group, value in late:
                acc = acc + jnp.where(group == g, value, 0.0)
            silu = acc / (1.0 + jnp.exp(-acc))
            out[g * rows : (g + 1) * rows, :] = silu.astype(jnp.bfloat16)
    first[...] = send_down(place_ref, 4, hidden, down, shape)
    for j in reversed(range(given.shape[0])):
        given[j] = send_down(place_ref, -1 - j, hidden, down, shape)


def last_body(place_ref, *refs):
    hidden, down, outs = refs[:2], refs[2:4], refs[4:]
    for j in reversed(range(len(outs))):
        outs[j][...] = send_down(place_ref, j, hidden, down, outs[j].shape)


def kernel(body, place, on_chip, stored, shapes, sems=0):
    vmem = pl.BlockSpec(memory_space=pltpu.VMEM)
    hbm = pl.BlockSpec(memory_space=pltpu.HBM)
    return pl.pallas_call(
        body,
        in_specs=[pl.BlockSpec(memory_space=pltpu.SMEM)]
        + [vmem] * len(on_chip)
        + [hbm] * len(stored),
        out_specs=[vmem] * len(shapes),
        out_shape=[jax.ShapeDtypeStruct(*shape) for shape in shapes],
        scratch_shapes=[pltpu.SemaphoreType.DMA((sems,))] if sems else [],
        compiler_params=pltpu.CompilerParams(vmem_limit_bytes=20 << 20),
    )(place, *on_chip, *stored)


def routing(routes, capacity, slot_count):
    token_count = routes.shape[0]
    expert_count = capacity.shape[0]
    expert_ids = jnp.arange(expert_count, dtype=jnp.int32)
    matches = routes[:, :, None] == expert_ids[None, None, :]
    named_count = matches.sum(axis=1).astype(jnp.bfloat16)
    token_ids = jnp.arange(token_count, dtype=jnp.int32)
    lower_mask = (token_ids[:, None] > token_ids[None, :]).astype(jnp.bfloat16)
    positions = jnp.dot(
        lower_mask, named_count, preferred_element_type=jnp.float32
    ).astype(jnp.int32)
    route_pos = jnp.sum(jnp.where(matches, positions[:, None, :], 0), axis=2)
    route_cap = jnp.sum(jnp.where(matches, capacity[None, None, :], 0), axis=2)
    kept_mask = route_pos < route_cap
    slot_index = jnp.where(kept_mask, routes * slot_count + route_pos, -1)
    slot_ids = jnp.arange(expert_count * slot_count, dtype=jnp.int32)
    dispatch = jnp.any(slot_ids[:, None, None] == slot_index[None, :, :], axis=2)
    return dispatch.astype(jnp.bfloat16), slot_index


def combining(slot_index, gate_num, total):
    first_share = gate_num.astype(jnp.float32) / 64.0
    weights = jnp.stack([first_share, 1.0 - first_share], axis=1)
    slot_ids = jnp.arange(total, dtype=jnp.int32)
    hits = slot_ids[None, :, None] == slot_index[:, None, :]
    return jnp.sum(jnp.where(hits, weights[:, None, :], 0.0), axis=2).astype(jnp.bfloat16)


def ring(value):
    count, low = lax.axis_size(CIRCLE), lax.axis_size("mp")

    def rank(y, core):
        return (y // low * 2 + core) * low + y % low

    pairs = [(rank(y, 0), rank((y + 1) % count, 0)) for y in range(count)]
    pairs += [(rank(y, 1), rank((y - 1) % count, 1)) for y in range(count)]
    return lax.ppermute(value, ("yh", "core", "mp"), pairs)


def swap(value):
    return lax.ppermute(value, "core", [(0, 1), (1, 0)])


def add(a, b):
    return (a.astype(jnp.float32) + b.astype(jnp.float32)).astype(jnp.bfloat16)


def per_device(tokens, routes, gate_num, capacity, w_up, w_down):
    expert_count = capacity.shape[0]
    token_count, width = tokens.shape
    slot_count = min(token_count, 3 * token_count // expert_count)
    half = lax.axis_size(CIRCLE) // 2
    place = jnp.stack([lax.axis_index(CIRCLE), 1 - 2 * lax.axis_index("core")])
    place, routes = lax.optimization_barrier((place.astype(jnp.int32), routes))
    up = w_up.T
    weights = (up, swap(up), w_down, swap(w_down))
    hidden_width = up.shape[0]
    dispatch, slot_index = routing(routes, capacity, slot_count)

    rows = jnp.dot(dispatch, tokens, preferred_element_type=jnp.float32).astype(jnp.bfloat16)
    arrived = lax.all_to_all(rows.reshape(expert_count, slot_count, width), "z", 0, 0, tiled=True)
    arrived, gate_num = lax.optimization_barrier((arrived, gate_num))
    combine = combining(slot_index, gate_num, expert_count * slot_count)
    mine = [arrived.reshape(expert_count * slot_count, width)]
    other = [swap(mine[0])]
    crossed = []
    for step in range(1, half + 1):
        mine.append(ring(mine[-1]))
        if step < half:
            other.append(ring(other[-1]))
            crossed.append(swap(other[-1]))

    chunk = (mine[0].shape, jnp.bfloat16)
    total_rows = 2 * mine[0].shape[0]
    sums = [((total_rows, hidden_width), jnp.float32)] * 2
    kept = [(weight.shape, weight.dtype) for weight in weights]
    *sum_refs, up_a, up_b = kernel(
        functools.partial(early_body, EARLY[0]), place, mine[:2], weights[:2], sums + kept[:2], 2
    )
    *sum_refs, down_a, down_b = kernel(
        functools.partial(early_body, EARLY[1]),
        place,
        [mine[2], *sum_refs, up_a, up_b],
        weights[2:],
        sums + kept[2:],
        2,
    )
    sum_refs = kernel(
        functools.partial(early_body, EARLY[2]),
        place,
        [crossed[0], mine[3], *sum_refs, up_a, up_b],
        [],
        sums,
    )
    first, given, *hidden = kernel(
        middle_body,
        place,
        [*sum_refs, mine[half], *crossed[1:], up_a, up_b, down_a, down_b],
        [],
        [chunk, ((half - 1, *chunk[0]), chunk[1])]
        + [((total_rows, hidden_width), jnp.bfloat16)] * 2,
    )
    own = kernel(last_body, place, [*hidden, down_a, down_b], [], [chunk] * half)
    own = [*own, first]

    taken = swap(given)
    mine_sum = ring(own[half])
    other_sum = ring(taken[half - 2])
    for step in range(half - 1, 0, -1):
        mine_sum = ring(add(own[step], mine_sum))
        if step > 1:
            other_sum = ring(add(taken[step - 2], other_sum))
    crossed_sum = swap(other_sum)

    total = own[0].astype(jnp.float32) + mine_sum.astype(jnp.float32)
    total = (total + crossed_sum.astype(jnp.float32)).astype(jnp.bfloat16)
    back = lax.all_to_all(
        total.reshape(expert_count, slot_count, width), "z", 0, 0, tiled=True
    )
    mixed = jnp.dot(
        combine,
        back.reshape(expert_count * slot_count, width),
        preferred_element_type=jnp.float32,
    )
    return mixed.astype(jnp.bfloat16)


def solution(mesh):
    sizes = dict(mesh.shape)
    group = sizes["expert"] // EXPERTS
    devices = mesh.devices.reshape(sizes["dp"], EXPERTS, group // 2, 2, sizes["mp"])
    fine = Mesh(devices, ("dp", "z", "yh", "core", "mp"))
    expert = ("z", "yh", "core")
    return jax.shard_map(
        per_device,
        mesh=fine,
        in_specs=(
            P(("dp", *expert), "mp"),
            P(("dp", *expert), None),
            P(("dp", *expert)),
            P(),
            P(None, (*expert, "mp")),
            P((*expert, "mp"), None),
        ),
        out_specs=P(("dp", *expert), "mp"),
        check_vma=False,
    )
```

```python
import functools

import jax
import jax.numpy as jnp
from jax import lax
from jax.experimental import pallas as pl
from jax.experimental.pallas import tpu as pltpu
from jax.sharding import Mesh, PartitionSpec as P


EXPERTS = 8
CIRCLE = ("yh", "mp")
EARLY = ((0, -1), (-2,), (1, 2, -3))
LATE = (-4, 3)


def spot(place_ref, offset, rows, width, features):
    chunks = features // width
    source = lax.rem(place_ref[0] + place_ref[1] * offset + 2 * chunks, 2 * chunks)
    row = pl.multiple_of(lax.div(source, chunks) * rows, rows)
    col = pl.multiple_of(lax.rem(source, chunks) * width, width)
    return lax.div(source, chunks), pl.ds(row, rows), pl.ds(col, width)


def projected(x, up):
    return lax.dot_general(x, up, (((1,), (1,)), ((), ())), preferred_element_type=jnp.float32)


def early_body(offsets, place_ref, *refs):
    refs = list(refs)
    first, sems = offsets is EARLY[0], refs.pop() if offsets is not EARLY[2] else None
    x_refs = [refs.pop(0) for _ in offsets]
    before = [] if first else [refs.pop(0) for _ in range(2)]
    up = [] if first else [refs.pop(0) for _ in range(2)]
    stored = [] if sems is None else [refs.pop(0) for _ in range(2)]
    sums, kept = refs[:2], refs[2:]
    copies = [
        pltpu.make_async_copy(src, dst, sems.at[i])
        for i, (src, dst) in enumerate(zip(stored, kept))
    ]
    for copy in copies:
        copy.start()
    for i, total in enumerate(sums):
        total[...] = jnp.zeros_like(total) if first else before[i][...]
    if first:
        up = kept
        for copy in copies:
            copy.wait()
    for x_ref, offset in zip(x_refs, offsets):
        _, rows, cols = spot(place_ref, offset, *x_ref.shape, up[0].shape[1])
        for total, up_ref in zip(sums, up):
            total[rows, :] += projected(x_ref[...], up_ref[:, cols])
    if not first:
        for copy in copies:
            copy.wait()


def send_down(place_ref, offset, hidden, down, shape):
    _, rows, cols = spot(place_ref, offset, *shape, down[0].shape[1])
    total = jnp.dot(hidden[0][rows, :], down[0][:, cols], preferred_element_type=jnp.float32)
    total += jnp.dot(hidden[1][rows, :], down[1][:, cols], preferred_element_type=jnp.float32)
    return total.astype(jnp.bfloat16)


def middle_body(place_ref, *refs):
    sums, x_refs, refs = refs[:2], refs[2 : 2 + len(LATE)], refs[2 + len(LATE) :]
    up, down, (first, given, *hidden) = refs[:2], refs[2:4], refs[4:]
    rows, width = shape = first.shape
    for total, up_ref, out in zip(sums, up, hidden):
        late = []
        for x_ref, offset in zip(x_refs, LATE):
            group, _, cols = spot(place_ref, offset, *shape, up_ref.shape[1])
            late.append((group, projected(x_ref[...], up_ref[:, cols])))
        for g in range(2):
            acc = total[g * rows : (g + 1) * rows, :]
            for group, value in late:
                acc = acc + jnp.where(group == g, value, 0.0)
            silu = acc / (1.0 + jnp.exp(-acc))
            out[g * rows : (g + 1) * rows, :] = silu.astype(jnp.bfloat16)
    first[...] = send_down(place_ref, 4, hidden, down, shape)
    for j in reversed(range(given.shape[0])):
        given[j] = send_down(place_ref, -1 - j, hidden, down, shape)


def last_body(place_ref, *refs):
    hidden, down, outs = refs[:2], refs[2:4], refs[4:]
    for j in reversed(range(len(outs))):
        outs[j][...] = send_down(place_ref, j, hidden, down, outs[j].shape)


def kernel(body, place, on_chip, stored, shapes, sems=0):
    vmem = pl.BlockSpec(memory_space=pltpu.VMEM)
    hbm = pl.BlockSpec(memory_space=pltpu.HBM)
    return pl.pallas_call(
        body,
        in_specs=[pl.BlockSpec(memory_space=pltpu.SMEM)]
        + [vmem] * len(on_chip)
        + [hbm] * len(stored),
        out_specs=[vmem] * len(shapes),
        out_shape=[jax.ShapeDtypeStruct(*shape) for shape in shapes],
        scratch_shapes=[pltpu.SemaphoreType.DMA((sems,))] if sems else [],
        compiler_params=pltpu.CompilerParams(vmem_limit_bytes=20 << 20),
    )(place, *on_chip, *stored)


def slots_of(routes, route_pos, route_cap, slot_count):
    return jnp.where(route_pos < route_cap, routes * slot_count + route_pos, -1)


def routing(routes, capacity, slot_count):
    token_count = routes.shape[0]
    expert_count = capacity.shape[0]
    expert_ids = jnp.arange(expert_count, dtype=jnp.int32)
    matches = routes[:, :, None] == expert_ids[None, None, :]
    named_count = matches.sum(axis=1).astype(jnp.bfloat16)
    token_ids = jnp.arange(token_count, dtype=jnp.int32)
    lower_mask = (token_ids[:, None] > token_ids[None, :]).astype(jnp.bfloat16)
    positions = jnp.dot(
        lower_mask, named_count, preferred_element_type=jnp.float32
    ).astype(jnp.int32)
    route_pos = jnp.sum(jnp.where(matches, positions[:, None, :], 0), axis=2)
    route_cap = jnp.sum(jnp.where(matches, capacity[None, None, :], 0), axis=2)
    slot_index = slots_of(routes, route_pos, route_cap, slot_count)
    slot_ids = jnp.arange(expert_count * slot_count, dtype=jnp.int32)
    dispatch = jnp.any(slot_ids[:, None, None] == slot_index[None, :, :], axis=2)
    return dispatch.astype(jnp.bfloat16), (routes, route_pos, route_cap)


def combining(slot_index, gate_num, total):
    first_share = gate_num.astype(jnp.float32) / 64.0
    weights = jnp.stack([first_share, 1.0 - first_share], axis=1)
    slot_ids = jnp.arange(total, dtype=jnp.int32)
    hits = slot_ids[None, :, None] == slot_index[:, None, :]
    return jnp.sum(jnp.where(hits, weights[:, None, :], 0.0), axis=2).astype(jnp.bfloat16)


def ring(value):
    count, low = lax.axis_size(CIRCLE), lax.axis_size("mp")

    def rank(y, core):
        return (y // low * 2 + core) * low + y % low

    pairs = [(rank(y, 0), rank((y + 1) % count, 0)) for y in range(count)]
    pairs += [(rank(y, 1), rank((y - 1) % count, 1)) for y in range(count)]
    return lax.ppermute(value, ("yh", "core", "mp"), pairs)


def swap(value):
    return lax.ppermute(value, "core", [(0, 1), (1, 0)])


def add(a, b):
    return (a.astype(jnp.float32) + b.astype(jnp.float32)).astype(jnp.bfloat16)


def per_device(tokens, routes, gate_num, capacity, w_up, w_down):
    expert_count = capacity.shape[0]
    token_count, width = tokens.shape
    slot_count = min(token_count, 3 * token_count // expert_count)
    half = lax.axis_size(CIRCLE) // 2
    place = jnp.stack([lax.axis_index(CIRCLE), 1 - 2 * lax.axis_index("core")])
    place, routes = lax.optimization_barrier((place.astype(jnp.int32), routes))
    up = w_up.T
    weights = (up, swap(up), w_down, swap(w_down))
    hidden_width = up.shape[0]
    dispatch, found = routing(routes, capacity, slot_count)

    rows = jnp.dot(dispatch, tokens, preferred_element_type=jnp.float32).astype(jnp.bfloat16)
    arrived = lax.all_to_all(rows.reshape(expert_count, slot_count, width), "z", 0, 0, tiled=True)
    arrived, gate_num, found = lax.optimization_barrier((arrived, gate_num, found))
    combine = combining(slots_of(*found, slot_count), gate_num, expert_count * slot_count)
    mine = [arrived.reshape(expert_count * slot_count, width)]
    other = [swap(mine[0])]
    crossed = []
    for step in range(1, half + 1):
        mine.append(ring(mine[-1]))
        if step < half:
            other.append(ring(other[-1]))
            crossed.append(swap(other[-1]))

    chunk = (mine[0].shape, jnp.bfloat16)
    total_rows = 2 * mine[0].shape[0]
    sums = [((total_rows, hidden_width), jnp.float32)] * 2
    kept = [(weight.shape, weight.dtype) for weight in weights]
    *sum_refs, up_a, up_b = kernel(
        functools.partial(early_body, EARLY[0]), place, mine[:2], weights[:2], sums + kept[:2], 2
    )
    *sum_refs, down_a, down_b = kernel(
        functools.partial(early_body, EARLY[1]),
        place,
        [mine[2], *sum_refs, up_a, up_b],
        weights[2:],
        sums + kept[2:],
        2,
    )
    sum_refs = kernel(
        functools.partial(early_body, EARLY[2]),
        place,
        [*crossed[:2], mine[3], *sum_refs, up_a, up_b],
        [],
        sums,
    )
    first, given, *hidden = kernel(
        middle_body,
        place,
        [*sum_refs, mine[half], *crossed[2:], up_a, up_b, down_a, down_b],
        [],
        [chunk, ((half - 1, *chunk[0]), chunk[1])]
        + [((total_rows, hidden_width), jnp.bfloat16)] * 2,
    )
    own = kernel(last_body, place, [*hidden, down_a, down_b], [], [chunk] * half)
    own = [*own, first]

    taken = swap(given)
    mine_sum = ring(own[half])
    other_sum = ring(taken[half - 2])
    for step in range(half - 1, 0, -1):
        mine_sum = ring(add(own[step], mine_sum))
        if step > 1:
            other_sum = ring(add(taken[step - 2], other_sum))
    crossed_sum = swap(other_sum)

    total = own[0].astype(jnp.float32) + mine_sum.astype(jnp.float32)
    total = (total + crossed_sum.astype(jnp.float32)).astype(jnp.bfloat16)
    back = lax.all_to_all(
        total.reshape(expert_count, slot_count, width), "z", 0, 0, tiled=True
    )
    mixed = jnp.dot(
        combine,
        back.reshape(expert_count * slot_count, width),
        preferred_element_type=jnp.float32,
    )
    return mixed.astype(jnp.bfloat16)


def solution(mesh):
    sizes = dict(mesh.shape)
    group = sizes["expert"] // EXPERTS
    devices = mesh.devices.reshape(sizes["dp"], EXPERTS, group // 2, 2, sizes["mp"])
    fine = Mesh(devices, ("dp", "z", "yh", "core", "mp"))
    expert = ("z", "yh", "core")
    return jax.shard_map(
        per_device,
        mesh=fine,
        in_specs=(
            P(("dp", *expert), "mp"),
            P(("dp", *expert), None),
            P(("dp", *expert)),
            P(),
            P(None, (*expert, "mp")),
            P((*expert, "mp"), None),
        ),
        out_specs=P(("dp", *expert), "mp"),
        check_vma=False,
    )
```

```python
import functools

import jax
import jax.numpy as jnp
from jax import lax
from jax.experimental import pallas as pl
from jax.experimental.pallas import tpu as pltpu
from jax.sharding import Mesh, PartitionSpec as P


EXPERTS = 8
CIRCLE = ("yh", "mp")
EARLY = ((0, -1), (-2,), (1, 2, -3))
LATE = (-4, 3)


def spot(place_ref, offset, rows, width, features):
    chunks = features // width
    source = lax.rem(place_ref[0] + place_ref[1] * offset + 2 * chunks, 2 * chunks)
    row = pl.multiple_of(lax.div(source, chunks) * rows, rows)
    col = pl.multiple_of(lax.rem(source, chunks) * width, width)
    return lax.div(source, chunks), pl.ds(row, rows), pl.ds(col, width)


def projected(x, up):
    return lax.dot_general(x, up, (((1,), (1,)), ((), ())), preferred_element_type=jnp.float32)


def early_body(offsets, place_ref, *refs):
    refs = list(refs)
    first, sems = offsets is EARLY[0], refs.pop() if offsets is not EARLY[2] else None
    x_refs = [refs.pop(0) for _ in offsets]
    before = [] if first else [refs.pop(0) for _ in range(2)]
    up = [] if first else [refs.pop(0) for _ in range(2)]
    stored = [] if sems is None else [refs.pop(0) for _ in range(2)]
    sums, kept = refs[:2], refs[2:]
    copies = [
        pltpu.make_async_copy(src, dst, sems.at[i])
        for i, (src, dst) in enumerate(zip(stored, kept))
    ]
    for copy in copies:
        copy.start()
    for i, total in enumerate(sums):
        total[...] = jnp.zeros_like(total) if first else before[i][...]
    if first:
        up = kept
        for copy in copies:
            copy.wait()
    for x_ref, offset in zip(x_refs, offsets):
        _, rows, cols = spot(place_ref, offset, *x_ref.shape, up[0].shape[1])
        for total, up_ref in zip(sums, up):
            total[rows, :] += projected(x_ref[...], up_ref[:, cols])
    if not first:
        for copy in copies:
            copy.wait()


def send_down(place_ref, offset, hidden, down, shape):
    _, rows, cols = spot(place_ref, offset, *shape, down[0].shape[1])
    total = jnp.dot(hidden[0][rows, :], down[0][:, cols], preferred_element_type=jnp.float32)
    total += jnp.dot(hidden[1][rows, :], down[1][:, cols], preferred_element_type=jnp.float32)
    return total.astype(jnp.bfloat16)


def middle_body(place_ref, *refs):
    sums, x_refs, refs = refs[:2], refs[2 : 2 + len(LATE)], refs[2 + len(LATE) :]
    up, down, (first, far, given, *hidden) = refs[:2], refs[2:4], refs[4:]
    rows, width = shape = first.shape
    for total, up_ref, out in zip(sums, up, hidden):
        late = []
        for x_ref, offset in zip(x_refs, LATE):
            group, _, cols = spot(place_ref, offset, *shape, up_ref.shape[1])
            late.append((group, projected(x_ref[...], up_ref[:, cols])))
        for g in range(2):
            acc = total[g * rows : (g + 1) * rows, :]
            for group, value in late:
                acc = acc + jnp.where(group == g, value, 0.0)
            silu = acc / (1.0 + jnp.exp(-acc))
            out[g * rows : (g + 1) * rows, :] = silu.astype(jnp.bfloat16)
    first[...] = send_down(place_ref, 4, hidden, down, shape)
    far[...] = send_down(place_ref, -3, hidden, down, shape)
    for j in reversed(range(given.shape[0])):
        given[j] = send_down(place_ref, -1 - j, hidden, down, shape)


def last_body(place_ref, *refs):
    hidden, down, outs = refs[:2], refs[2:4], refs[4:]
    for j in reversed(range(len(outs))):
        outs[j][...] = send_down(place_ref, j, hidden, down, outs[j].shape)


def kernel(body, place, on_chip, stored, shapes, sems=0):
    vmem = pl.BlockSpec(memory_space=pltpu.VMEM)
    hbm = pl.BlockSpec(memory_space=pltpu.HBM)
    return pl.pallas_call(
        body,
        in_specs=[pl.BlockSpec(memory_space=pltpu.SMEM)]
        + [vmem] * len(on_chip)
        + [hbm] * len(stored),
        out_specs=[vmem] * len(shapes),
        out_shape=[jax.ShapeDtypeStruct(*shape) for shape in shapes],
        scratch_shapes=[pltpu.SemaphoreType.DMA((sems,))] if sems else [],
        compiler_params=pltpu.CompilerParams(vmem_limit_bytes=20 << 20),
    )(place, *on_chip, *stored)


def slots_of(routes, route_pos, route_cap, slot_count):
    return jnp.where(route_pos < route_cap, routes * slot_count + route_pos, -1)


def routing(routes, capacity, slot_count):
    token_count = routes.shape[0]
    expert_count = capacity.shape[0]
    expert_ids = jnp.arange(expert_count, dtype=jnp.int32)
    matches = routes[:, :, None] == expert_ids[None, None, :]
    named_count = matches.sum(axis=1).astype(jnp.bfloat16)
    token_ids = jnp.arange(token_count, dtype=jnp.int32)
    lower_mask = (token_ids[:, None] > token_ids[None, :]).astype(jnp.bfloat16)
    positions = jnp.dot(
        lower_mask, named_count, preferred_element_type=jnp.float32
    ).astype(jnp.int32)
    route_pos = jnp.sum(jnp.where(matches, positions[:, None, :], 0), axis=2)
    route_cap = jnp.sum(jnp.where(matches, capacity[None, None, :], 0), axis=2)
    slot_index = slots_of(routes, route_pos, route_cap, slot_count)
    slot_ids = jnp.arange(expert_count * slot_count, dtype=jnp.int32)
    dispatch = jnp.any(slot_ids[:, None, None] == slot_index[None, :, :], axis=2)
    return dispatch.astype(jnp.bfloat16), (routes, route_pos, route_cap)


def combining(slot_index, gate_num, total):
    first_share = gate_num.astype(jnp.float32) / 64.0
    weights = jnp.stack([first_share, 1.0 - first_share], axis=1)
    slot_ids = jnp.arange(total, dtype=jnp.int32)
    hits = slot_ids[None, :, None] == slot_index[:, None, :]
    return jnp.sum(jnp.where(hits, weights[:, None, :], 0.0), axis=2).astype(jnp.bfloat16)


def ring(value, leave=False):
    count, low = lax.axis_size(CIRCLE), lax.axis_size("mp")

    def rank(y, core):
        return (y // low * 2 + core) * low + y % low

    pairs = [
        (rank(y, way ^ leave), rank((y + 1 - 2 * way) % count, way))
        for way in range(2)
        for y in range(count)
    ]
    return lax.ppermute(value, ("yh", "core", "mp"), pairs)


def swap(value):
    return lax.ppermute(value, "core", [(0, 1), (1, 0)])


def add(a, b):
    return (a.astype(jnp.float32) + b.astype(jnp.float32)).astype(jnp.bfloat16)


def per_device(tokens, routes, gate_num, capacity, w_up, w_down):
    expert_count = capacity.shape[0]
    token_count, width = tokens.shape
    slot_count = min(token_count, 3 * token_count // expert_count)
    half = lax.axis_size(CIRCLE) // 2
    place = jnp.stack([lax.axis_index(CIRCLE), 1 - 2 * lax.axis_index("core")])
    place, routes = lax.optimization_barrier((place.astype(jnp.int32), routes))
    up = w_up.T
    weights = (up, swap(up), w_down, swap(w_down))
    hidden_width = up.shape[0]
    dispatch, found = routing(routes, capacity, slot_count)

    rows = jnp.dot(dispatch, tokens, preferred_element_type=jnp.float32).astype(jnp.bfloat16)
    arrived = lax.all_to_all(rows.reshape(expert_count, slot_count, width), "z", 0, 0, tiled=True)
    arrived, gate_num, found = lax.optimization_barrier((arrived, gate_num, found))
    combine = combining(slots_of(*found, slot_count), gate_num, expert_count * slot_count)
    mine = [arrived.reshape(expert_count * slot_count, width)]
    other = [swap(mine[0])]
    crossed = []
    for step in range(1, half + 1):
        mine.append(ring(mine[-1]))
        if step < half:
            other.append(ring(other[-1]))
            crossed.append(swap(other[-1]))

    chunk = (mine[0].shape, jnp.bfloat16)
    total_rows = 2 * mine[0].shape[0]
    sums = [((total_rows, hidden_width), jnp.float32)] * 2
    kept = [(weight.shape, weight.dtype) for weight in weights]
    *sum_refs, up_a, up_b = kernel(
        functools.partial(early_body, EARLY[0]), place, mine[:2], weights[:2], sums + kept[:2], 2
    )
    *sum_refs, down_a, down_b = kernel(
        functools.partial(early_body, EARLY[1]),
        place,
        [mine[2], *sum_refs, up_a, up_b],
        weights[2:],
        sums + kept[2:],
        2,
    )
    sum_refs = kernel(
        functools.partial(early_body, EARLY[2]),
        place,
        [*crossed[:2], mine[3], *sum_refs, up_a, up_b],
        [],
        sums,
    )
    first, far, given, *hidden = kernel(
        middle_body,
        place,
        [*sum_refs, mine[half], *crossed[2:], up_a, up_b, down_a, down_b],
        [],
        [chunk, chunk, ((half - 2, *chunk[0]), chunk[1])]
        + [((total_rows, hidden_width), jnp.bfloat16)] * 2,
    )
    own = kernel(last_body, place, [*hidden, down_a, down_b], [], [chunk] * half)
    own = [*own, first]

    taken = swap(given)
    mine_sum = ring(own[half])
    other_sum = ring(far, leave=True)
    for step in range(half - 1, 0, -1):
        mine_sum = ring(add(own[step], mine_sum))
        if step > 1:
            other_sum = ring(add(taken[step - 2], other_sum))
    crossed_sum = swap(other_sum)

    total = own[0].astype(jnp.float32) + mine_sum.astype(jnp.float32)
    total = (total + crossed_sum.astype(jnp.float32)).astype(jnp.bfloat16)
    back = lax.all_to_all(
        total.reshape(expert_count, slot_count, width), "z", 0, 0, tiled=True
    )
    mixed = jnp.dot(
        combine,
        back.reshape(expert_count * slot_count, width),
        preferred_element_type=jnp.float32,
    )
    return mixed.astype(jnp.bfloat16)


def solution(mesh):
    sizes = dict(mesh.shape)
    group = sizes["expert"] // EXPERTS
    devices = mesh.devices.reshape(sizes["dp"], EXPERTS, group // 2, 2, sizes["mp"])
    fine = Mesh(devices, ("dp", "z", "yh", "core", "mp"))
    expert = ("z", "yh", "core")
    return jax.shard_map(
        per_device,
        mesh=fine,
        in_specs=(
            P(("dp", *expert), "mp"),
            P(("dp", *expert), None),
            P(("dp", *expert)),
            P(),
            P(None, (*expert, "mp")),
            P((*expert, "mp"), None),
        ),
        out_specs=P(("dp", *expert), "mp"),
        check_vma=False,
    )
```

```python
import functools

import jax
import jax.numpy as jnp
from jax import lax
from jax.experimental import pallas as pl
from jax.experimental.pallas import tpu as pltpu
from jax.sharding import Mesh, PartitionSpec as P


EXPERTS = 8
CIRCLE = ("yh", "mp")
EARLY = ((0, -1), (-2,), (1, 2, -3))
LATE = (-4, 3)


def spot(place_ref, offset, rows, width, features):
    chunks = features // width
    source = lax.rem(place_ref[0] + place_ref[1] * offset + 2 * chunks, 2 * chunks)
    row = pl.multiple_of(lax.div(source, chunks) * rows, rows)
    col = pl.multiple_of(lax.rem(source, chunks) * width, width)
    return lax.div(source, chunks), pl.ds(row, rows), pl.ds(col, width)


def projected(x, up):
    return lax.dot_general(x, up, (((1,), (1,)), ((), ())), preferred_element_type=jnp.float32)


def early_body(offsets, place_ref, *refs):
    refs = list(refs)
    first, sems = offsets is EARLY[0], refs.pop() if offsets is not EARLY[2] else None
    x_refs = [refs.pop(0) for _ in offsets]
    before = [] if first else [refs.pop(0) for _ in range(2)]
    up = [] if first else [refs.pop(0) for _ in range(2)]
    stored = [] if sems is None else [refs.pop(0) for _ in range(2)]
    sums, kept = refs[:2], refs[2:]
    copies = [
        pltpu.make_async_copy(src, dst, sems.at[i])
        for i, (src, dst) in enumerate(zip(stored, kept))
    ]
    for copy in copies:
        copy.start()
    for i, total in enumerate(sums):
        total[...] = jnp.zeros_like(total) if first else before[i][...]
    if first:
        up = kept
        for copy in copies:
            copy.wait()
    for x_ref, offset in zip(x_refs, offsets):
        _, rows, cols = spot(place_ref, offset, *x_ref.shape, up[0].shape[1])
        for total, up_ref in zip(sums, up):
            total[rows, :] += projected(x_ref[...], up_ref[:, cols])
    if not first:
        for copy in copies:
            copy.wait()


def send_down(place_ref, offset, hidden, down, shape):
    _, rows, cols = spot(place_ref, offset, *shape, down[0].shape[1])
    total = jnp.dot(hidden[0][rows, :], down[0][:, cols], preferred_element_type=jnp.float32)
    total += jnp.dot(hidden[1][rows, :], down[1][:, cols], preferred_element_type=jnp.float32)
    return total.astype(jnp.bfloat16)


def middle_body(place_ref, *refs):
    sums, x_refs, refs = refs[:2], refs[2 : 2 + len(LATE)], refs[2 + len(LATE) :]
    up, down, (first, far, given, *hidden) = refs[:2], refs[2:4], refs[4:]
    rows, width = shape = first.shape
    for total, up_ref, out in zip(sums, up, hidden):
        late = []
        for x_ref, offset in zip(x_refs, LATE):
            group, _, cols = spot(place_ref, offset, *shape, up_ref.shape[1])
            late.append((group, projected(x_ref[...], up_ref[:, cols])))
        for g in range(2):
            acc = total[g * rows : (g + 1) * rows, :]
            for group, value in late:
                acc = acc + jnp.where(group == g, value, 0.0)
            silu = acc / (1.0 + jnp.exp(-acc))
            out[g * rows : (g + 1) * rows, :] = silu.astype(jnp.bfloat16)
    first[...] = send_down(place_ref, 4, hidden, down, shape)
    far[...] = send_down(place_ref, -3, hidden, down, shape)
    for j in reversed(range(given.shape[0])):
        given[j] = send_down(place_ref, -1 - j, hidden, down, shape)


def last_body(place_ref, *refs):
    hidden, down, outs = refs[:2], refs[2:4], refs[4:]
    for j in reversed(range(len(outs))):
        outs[j][...] = send_down(place_ref, j, hidden, down, outs[j].shape)


def kernel(body, place, on_chip, stored, shapes, sems=0):
    vmem = pl.BlockSpec(memory_space=pltpu.VMEM)
    hbm = pl.BlockSpec(memory_space=pltpu.HBM)
    return pl.pallas_call(
        body,
        in_specs=[pl.BlockSpec(memory_space=pltpu.SMEM)]
        + [vmem] * len(on_chip)
        + [hbm] * len(stored),
        out_specs=[vmem] * len(shapes),
        out_shape=[jax.ShapeDtypeStruct(*shape) for shape in shapes],
        scratch_shapes=[pltpu.SemaphoreType.DMA((sems,))] if sems else [],
        compiler_params=pltpu.CompilerParams(vmem_limit_bytes=20 << 20),
    )(place, *on_chip, *stored)


def slots_of(routes, route_pos, route_cap, slot_count):
    return jnp.where(route_pos < route_cap, routes * slot_count + route_pos, -1)


def routing(routes, capacity, slot_count):
    token_count = routes.shape[0]
    expert_count = capacity.shape[0]
    expert_ids = jnp.arange(expert_count, dtype=jnp.int32)
    matches = routes[:, :, None] == expert_ids[None, None, :]
    named_count = matches.sum(axis=1).astype(jnp.bfloat16)
    token_ids = jnp.arange(token_count, dtype=jnp.int32)
    lower_mask = (token_ids[:, None] > token_ids[None, :]).astype(jnp.bfloat16)
    positions = jnp.dot(
        lower_mask, named_count, preferred_element_type=jnp.float32
    ).astype(jnp.int32)
    route_pos = jnp.sum(jnp.where(matches, positions[:, None, :], 0), axis=2)
    route_cap = jnp.sum(jnp.where(matches, capacity[None, None, :], 0), axis=2)
    slot_index = slots_of(routes, route_pos, route_cap, slot_count)
    slot_ids = jnp.arange(expert_count * slot_count, dtype=jnp.int32)
    dispatch = jnp.any(slot_ids[:, None, None] == slot_index[None, :, :], axis=2)
    return dispatch.astype(jnp.bfloat16), (routes, route_pos, route_cap)


def combining(slot_index, gate_num, total):
    first_share = gate_num.astype(jnp.float32) / 64.0
    weights = jnp.stack([first_share, 1.0 - first_share], axis=1)
    slot_ids = jnp.arange(total, dtype=jnp.int32)
    hits = slot_ids[None, :, None] == slot_index[:, None, :]
    return jnp.sum(jnp.where(hits, weights[:, None, :], 0.0), axis=2).astype(jnp.bfloat16)


def ring(value, leave=False):
    count, low = lax.axis_size(CIRCLE), lax.axis_size("mp")

    def rank(y, core):
        return (y // low * 2 + core) * low + y % low

    pairs = [
        (rank(y, way ^ leave), rank((y + 1 - 2 * way) % count, way))
        for way in range(2)
        for y in range(count)
    ]
    return lax.ppermute(value, ("yh", "core", "mp"), pairs)


def swap(value):
    return lax.ppermute(value, "core", [(0, 1), (1, 0)])


def add(a, b):
    return (a.astype(jnp.float32) + b.astype(jnp.float32)).astype(jnp.bfloat16)


def per_device(tokens, routes, gate_num, capacity, w_up, w_down):
    expert_count = capacity.shape[0]
    token_count, width = tokens.shape
    slot_count = min(token_count, 3 * token_count // expert_count)
    half = lax.axis_size(CIRCLE) // 2
    place = jnp.stack([lax.axis_index(CIRCLE), 1 - 2 * lax.axis_index("core")])
    place, routes = lax.optimization_barrier((place.astype(jnp.int32), routes))
    up = w_up.T
    weights = (up, swap(up), w_down, swap(w_down))
    hidden_width = up.shape[0]
    dispatch, found = routing(routes, capacity, slot_count)

    rows = jnp.dot(dispatch, tokens, preferred_element_type=jnp.float32).astype(jnp.bfloat16)
    arrived = lax.all_to_all(rows.reshape(expert_count, slot_count, width), "z", 0, 0, tiled=True)
    arrived, gate_num, found = lax.optimization_barrier((arrived, gate_num, found))
    combine = combining(slots_of(*found, slot_count), gate_num, expert_count * slot_count)
    mine = [arrived.reshape(expert_count * slot_count, width)]
    other, crossed = mine[0], []
    for step in range(1, half + 1):
        mine.append(ring(mine[-1]))
        if step < half:
            other = ring(other, leave=step == 1)
            crossed.append(swap(other))

    chunk = (mine[0].shape, jnp.bfloat16)
    total_rows = 2 * mine[0].shape[0]
    sums = [((total_rows, hidden_width), jnp.float32)] * 2
    kept = [(weight.shape, weight.dtype) for weight in weights]
    *sum_refs, up_a, up_b = kernel(
        functools.partial(early_body, EARLY[0]), place, mine[:2], weights[:2], sums + kept[:2], 2
    )
    *sum_refs, down_a, down_b = kernel(
        functools.partial(early_body, EARLY[1]),
        place,
        [mine[2], *sum_refs, up_a, up_b],
        weights[2:],
        sums + kept[2:],
        2,
    )
    sum_refs = kernel(
        functools.partial(early_body, EARLY[2]),
        place,
        [*crossed[:2], mine[3], *sum_refs, up_a, up_b],
        [],
        sums,
    )
    first, far, given, *hidden = kernel(
        middle_body,
        place,
        [*sum_refs, mine[half], *crossed[2:], up_a, up_b, down_a, down_b],
        [],
        [chunk, chunk, ((half - 2, *chunk[0]), chunk[1])]
        + [((total_rows, hidden_width), jnp.bfloat16)] * 2,
    )
    own = kernel(last_body, place, [*hidden, down_a, down_b], [], [chunk] * half)
    own = [*own, first]

    taken = swap(given)
    mine_sum = ring(own[half])
    other_sum = ring(far, leave=True)
    for step in range(half - 1, 0, -1):
        mine_sum = ring(add(own[step], mine_sum))
        if step > 1:
            other_sum = ring(add(taken[step - 2], other_sum))
    crossed_sum = swap(other_sum)

    total = own[0].astype(jnp.float32) + mine_sum.astype(jnp.float32)
    total = (total + crossed_sum.astype(jnp.float32)).astype(jnp.bfloat16)
    back = lax.all_to_all(
        total.reshape(expert_count, slot_count, width), "z", 0, 0, tiled=True
    )
    mixed = jnp.dot(
        combine,
        back.reshape(expert_count * slot_count, width),
        preferred_element_type=jnp.float32,
    )
    return mixed.astype(jnp.bfloat16)


def solution(mesh):
    sizes = dict(mesh.shape)
    group = sizes["expert"] // EXPERTS
    devices = mesh.devices.reshape(sizes["dp"], EXPERTS, group // 2, 2, sizes["mp"])
    fine = Mesh(devices, ("dp", "z", "yh", "core", "mp"))
    expert = ("z", "yh", "core")
    return jax.shard_map(
        per_device,
        mesh=fine,
        in_specs=(
            P(("dp", *expert), "mp"),
            P(("dp", *expert), None),
            P(("dp", *expert)),
            P(),
            P(None, (*expert, "mp")),
            P((*expert, "mp"), None),
        ),
        out_specs=P(("dp", *expert), "mp"),
        check_vma=False,
    )
```

```python
import functools

import jax
import jax.numpy as jnp
from jax import lax
from jax.experimental import pallas as pl
from jax.experimental.pallas import tpu as pltpu
from jax.sharding import Mesh, PartitionSpec as P


EXPERTS = 8
CIRCLE = ("yh", "mp")
EARLY = ((0, -1), (-2,), (1, 2, -3))
LATE = (-4, 3)


def spot(place_ref, offset, rows, width, features):
    chunks = features // width
    source = lax.rem(place_ref[0] + place_ref[1] * offset + 2 * chunks, 2 * chunks)
    row = pl.multiple_of(lax.div(source, chunks) * rows, rows)
    col = pl.multiple_of(lax.rem(source, chunks) * width, width)
    return lax.div(source, chunks), pl.ds(row, rows), pl.ds(col, width)


def projected(x, up):
    return lax.dot_general(x, up, (((1,), (1,)), ((), ())), preferred_element_type=jnp.float32)


def early_body(offsets, place_ref, *refs):
    refs = list(refs)
    first, sems = offsets is EARLY[0], refs.pop() if offsets is not EARLY[2] else None
    x_refs = [refs.pop(0) for _ in offsets]
    before = [] if first else [refs.pop(0) for _ in range(2)]
    up = [] if first else [refs.pop(0) for _ in range(2)]
    stored = [] if sems is None else [refs.pop(0) for _ in range(2)]
    sums, kept = refs[:2], refs[2:]
    copies = [
        pltpu.make_async_copy(src, dst, sems.at[i])
        for i, (src, dst) in enumerate(zip(stored, kept))
    ]
    for copy in copies:
        copy.start()
    for i, total in enumerate(sums):
        total[...] = jnp.zeros_like(total) if first else before[i][...]
    if first:
        up = kept
        for copy in copies:
            copy.wait()
    for x_ref, offset in zip(x_refs, offsets):
        _, rows, cols = spot(place_ref, offset, *x_ref.shape, up[0].shape[1])
        for total, up_ref in zip(sums, up):
            total[rows, :] += projected(x_ref[...], up_ref[:, cols])
    if not first:
        for copy in copies:
            copy.wait()


def send_down(place_ref, offset, hidden, down, shape):
    _, rows, cols = spot(place_ref, offset, *shape, down[0].shape[1])
    total = jnp.dot(hidden[0][rows, :], down[0][:, cols], preferred_element_type=jnp.float32)
    total += jnp.dot(hidden[1][rows, :], down[1][:, cols], preferred_element_type=jnp.float32)
    return total.astype(jnp.bfloat16)


def middle_body(place_ref, *refs):
    sums, x_refs, refs = refs[:2], refs[2 : 2 + len(LATE)], refs[2 + len(LATE) :]
    up, down, (first, far, *hidden) = refs[:2], refs[2:4], refs[4:]
    rows, width = shape = first.shape
    for total, up_ref, out in zip(sums, up, hidden):
        late = []
        for x_ref, offset in zip(x_refs, LATE):
            group, _, cols = spot(place_ref, offset, *shape, up_ref.shape[1])
            late.append((group, projected(x_ref[...], up_ref[:, cols])))
        for g in range(2):
            acc = total[g * rows : (g + 1) * rows, :]
            for group, value in late:
                acc = acc + jnp.where(group == g, value, 0.0)
            silu = acc / (1.0 + jnp.exp(-acc))
            out[g * rows : (g + 1) * rows, :] = silu.astype(jnp.bfloat16)
    first[...] = send_down(place_ref, 4, hidden, down, shape)
    far[...] = send_down(place_ref, -3, hidden, down, shape)


def given_body(place_ref, *refs):
    hidden, down, given = refs[:2], refs[2:4], refs[4]
    for j in reversed(range(given.shape[0])):
        given[j] = send_down(place_ref, -1 - j, hidden, down, given.shape[1:])


def last_body(place_ref, *refs):
    hidden, down, outs = refs[:2], refs[2:4], refs[4:]
    for j in reversed(range(len(outs))):
        outs[j][...] = send_down(place_ref, j, hidden, down, outs[j].shape)


def kernel(body, place, on_chip, stored, shapes, sems=0):
    vmem = pl.BlockSpec(memory_space=pltpu.VMEM)
    hbm = pl.BlockSpec(memory_space=pltpu.HBM)
    return pl.pallas_call(
        body,
        in_specs=[pl.BlockSpec(memory_space=pltpu.SMEM)]
        + [vmem] * len(on_chip)
        + [hbm] * len(stored),
        out_specs=[vmem] * len(shapes),
        out_shape=[jax.ShapeDtypeStruct(*shape) for shape in shapes],
        scratch_shapes=[pltpu.SemaphoreType.DMA((sems,))] if sems else [],
        compiler_params=pltpu.CompilerParams(vmem_limit_bytes=20 << 20),
    )(place, *on_chip, *stored)


def slots_of(routes, route_pos, route_cap, slot_count):
    return jnp.where(route_pos < route_cap, routes * slot_count + route_pos, -1)


def routing(routes, capacity, slot_count):
    token_count = routes.shape[0]
    expert_count = capacity.shape[0]
    expert_ids = jnp.arange(expert_count, dtype=jnp.int32)
    matches = routes[:, :, None] == expert_ids[None, None, :]
    named_count = matches.sum(axis=1).astype(jnp.bfloat16)
    token_ids = jnp.arange(token_count, dtype=jnp.int32)
    lower_mask = (token_ids[:, None] > token_ids[None, :]).astype(jnp.bfloat16)
    positions = jnp.dot(
        lower_mask, named_count, preferred_element_type=jnp.float32
    ).astype(jnp.int32)
    route_pos = jnp.sum(jnp.where(matches, positions[:, None, :], 0), axis=2)
    route_cap = jnp.sum(jnp.where(matches, capacity[None, None, :], 0), axis=2)
    slot_index = slots_of(routes, route_pos, route_cap, slot_count)
    slot_ids = jnp.arange(expert_count * slot_count, dtype=jnp.int32)
    dispatch = jnp.any(slot_ids[:, None, None] == slot_index[None, :, :], axis=2)
    return dispatch.astype(jnp.bfloat16), (routes, route_pos, route_cap)


def combining(slot_index, gate_num, total):
    first_share = gate_num.astype(jnp.float32) / 64.0
    weights = jnp.stack([first_share, 1.0 - first_share], axis=1)
    slot_ids = jnp.arange(total, dtype=jnp.int32)
    hits = slot_ids[None, :, None] == slot_index[:, None, :]
    return jnp.sum(jnp.where(hits, weights[:, None, :], 0.0), axis=2).astype(jnp.bfloat16)


def ring(value, leave=False):
    count, low = lax.axis_size(CIRCLE), lax.axis_size("mp")

    def rank(y, core):
        return (y // low * 2 + core) * low + y % low

    pairs = [
        (rank(y, way ^ leave), rank((y + 1 - 2 * way) % count, way))
        for way in range(2)
        for y in range(count)
    ]
    return lax.ppermute(value, ("yh", "core", "mp"), pairs)


def swap(value):
    return lax.ppermute(value, "core", [(0, 1), (1, 0)])


def add(a, b):
    return (a.astype(jnp.float32) + b.astype(jnp.float32)).astype(jnp.bfloat16)


def per_device(tokens, routes, gate_num, capacity, w_up, w_down):
    expert_count = capacity.shape[0]
    token_count, width = tokens.shape
    slot_count = min(token_count, 3 * token_count // expert_count)
    half = lax.axis_size(CIRCLE) // 2
    place = jnp.stack([lax.axis_index(CIRCLE), 1 - 2 * lax.axis_index("core")])
    place, routes = lax.optimization_barrier((place.astype(jnp.int32), routes))
    up = w_up.T
    weights = (up, swap(up), w_down, swap(w_down))
    hidden_width = up.shape[0]
    dispatch, found = routing(routes, capacity, slot_count)

    rows = jnp.dot(dispatch, tokens, preferred_element_type=jnp.float32).astype(jnp.bfloat16)
    arrived = lax.all_to_all(rows.reshape(expert_count, slot_count, width), "z", 0, 0, tiled=True)
    arrived, gate_num, found = lax.optimization_barrier((arrived, gate_num, found))
    combine = combining(slots_of(*found, slot_count), gate_num, expert_count * slot_count)
    mine = [arrived.reshape(expert_count * slot_count, width)]
    other = [swap(mine[0])]
    crossed = []
    for step in range(1, half + 1):
        mine.append(ring(mine[-1]))
        if step < half:
            other.append(ring(other[-1]))
            crossed.append(swap(other[-1]))

    chunk = (mine[0].shape, jnp.bfloat16)
    total_rows = 2 * mine[0].shape[0]
    sums = [((total_rows, hidden_width), jnp.float32)] * 2
    kept = [(weight.shape, weight.dtype) for weight in weights]
    *sum_refs, up_a, up_b = kernel(
        functools.partial(early_body, EARLY[0]), place, mine[:2], weights[:2], sums + kept[:2], 2
    )
    *sum_refs, down_a, down_b = kernel(
        functools.partial(early_body, EARLY[1]),
        place,
        [mine[2], *sum_refs, up_a, up_b],
        weights[2:],
        sums + kept[2:],
        2,
    )
    sum_refs = kernel(
        functools.partial(early_body, EARLY[2]),
        place,
        [*crossed[:2], mine[3], *sum_refs, up_a, up_b],
        [],
        sums,
    )
    first, far, *hidden = kernel(
        middle_body,
        place,
        [*sum_refs, mine[half], *crossed[2:], up_a, up_b, down_a, down_b],
        [],
        [chunk, chunk] + [((total_rows, hidden_width), jnp.bfloat16)] * 2,
    )
    given_shape = ((half - 2, *chunk[0]), chunk[1])
    (given,) = kernel(given_body, place, [*hidden, down_a, down_b], [], [given_shape])
    own = kernel(last_body, place, [*hidden, down_a, down_b], [], [chunk] * half)
    own = [*own, first]

    taken = swap(given)
    mine_sum = ring(own[half])
    other_sum = ring(far, leave=True)
    for step in range(half - 1, 0, -1):
        mine_sum = ring(add(own[step], mine_sum))
        if step > 1:
            other_sum = ring(add(taken[step - 2], other_sum))
    crossed_sum = swap(other_sum)

    total = own[0].astype(jnp.float32) + mine_sum.astype(jnp.float32)
    total = (total + crossed_sum.astype(jnp.float32)).astype(jnp.bfloat16)
    back = lax.all_to_all(
        total.reshape(expert_count, slot_count, width), "z", 0, 0, tiled=True
    )
    mixed = jnp.dot(
        combine,
        back.reshape(expert_count * slot_count, width),
        preferred_element_type=jnp.float32,
    )
    return mixed.astype(jnp.bfloat16)


def solution(mesh):
    sizes = dict(mesh.shape)
    group = sizes["expert"] // EXPERTS
    devices = mesh.devices.reshape(sizes["dp"], EXPERTS, group // 2, 2, sizes["mp"])
    fine = Mesh(devices, ("dp", "z", "yh", "core", "mp"))
    expert = ("z", "yh", "core")
    return jax.shard_map(
        per_device,
        mesh=fine,
        in_specs=(
            P(("dp", *expert), "mp"),
            P(("dp", *expert), None),
            P(("dp", *expert)),
            P(),
            P(None, (*expert, "mp")),
            P((*expert, "mp"), None),
        ),
        out_specs=P(("dp", *expert), "mp"),
        check_vma=False,
    )
```
